512 devices in a mesh: row: 16 (over x_hi, y, core), col: 32 (over x_lo, z).
Axes of the slice: x: 4 (x_hi: 2, x_lo: 2; x = x_hi * 2 + x_lo), y: 4, z: 16, core: 2. Of those that a mesh axis runs over, the one named last changes fastest.
Arguments:
- velocity_modes: bfloat16 [3, 176, 352, 704], P(None, 'row', 'col'), may hold values from -0.00090789795 to 0.00090789795
- wavenumbers: float32 [8], replicated, may hold values from 0.5 to 3
- polar: float32 [32], replicated, may hold values from -3.140625 to 3.140625
- azimuth: float32 [32], replicated, may hold values from -3.140625 to 3.140625
Outputs:
- velocity: bfloat16 [3, 512, 512, 512], P(None, 'row', 'col')
- far_field: float32 [32, 2, 8], P('col')
The draws below stay inside these ranges and needn't reach their ends.
All inputs are finite; a program needn't handle non-finite values.
Results may differ from the reference program's by a relative error of at most 0.0075.
Values may be sent and summed in bfloat16 or wider, within the bound.
A program may use at most 64 MiB of HBM per device.

```python
import math
import jax
import jax.numpy as jnp
from jax import lax

N = 512
M = 352
KX = 176
FREQS = 8
DIRS = 32


def levels(rng, extent, split, low, largest):
    factor_of, own = 1.0, jax.random.fold_in(rng, 6)
    for axis_at, blocks in split:
        draws = jnp.exp(jax.random.uniform(jax.random.fold_in(own, axis_at), (blocks,), jnp.float32, low / len(split), largest / len(split)))
        factor_of = factor_of * jnp.repeat(draws, extent[axis_at] // blocks).reshape([-1 if axis == axis_at else 1 for axis in range(len(extent))])
    return factor_of


def scatter_about(key, shape, width, most, cuts=(), kind=jnp.bfloat16):
    factor_of = levels(key, shape, cuts, -0.22, 0.18) if cuts else 1.0
    drawn = jax.random.normal(key, shape, jnp.float32) * width * factor_of
    return jnp.minimum(jnp.maximum(drawn, -most), most).astype(kind)


def setup_inputs(seed: int = 0) -> dict:
    streams_of = jax.random.split(jax.random.key(seed), 5)
    return {
        "velocity_modes": scatter_about(streams_of[0], (3, KX, M, 2 * M), (M ** -1.5), 0.00090789795, ((1, 16), (2, 32))),
        "wavenumbers": jnp.clip(jnp.exp(jax.random.uniform(streams_of[1], (FREQS,), jnp.float32, math.log(0.5), math.log(3.0))), 0.5, 3.0),
        "polar": jnp.clip(jax.random.uniform(streams_of[2], (DIRS,), jnp.float32, -3.140625, 3.140625), -3.140625, 3.140625),
        "azimuth": jnp.clip(jax.random.uniform(streams_of[3], (DIRS,), jnp.float32, -3.140625, 3.140625), -3.140625, 3.140625),
    }


def complex_table(modes, points):
    waves = jnp.arange(modes, dtype=jnp.int32) - modes // 2
    cells = jnp.arange(points, dtype=jnp.int32)
    product = jnp.mod(waves[:, None] * cells[None, :], points)
    angle = product.astype(jnp.float32) * (2.0 * math.pi / points)
    cosine = jnp.cos(angle)
    sine = jnp.sin(angle)
    table = jnp.stack([jnp.stack([cosine, sine], 1), jnp.stack([-sine, cosine], 1)], 0)
    return table.astype(jnp.bfloat16)


def half_table(count, points):
    waves = jnp.arange(count, dtype=jnp.int32)
    cells = jnp.arange(points, dtype=jnp.int32)
    product = jnp.mod(waves[:, None] * cells[None, :], points)
    angle = product.astype(jnp.float32) * (2.0 * math.pi / points)
    cosine = jnp.cos(angle).astype(jnp.bfloat16)
    sine = jnp.sin(angle).astype(jnp.bfloat16)
    factor = jnp.where(waves == 0, 1.0, 2.0).astype(jnp.bfloat16)[:, None]
    return jnp.stack([factor * cosine, -(factor * sine)], 0)


def stresses(field):
    trace = (field[0] * field[0] + field[1] * field[1] + field[2] * field[2]) / 3.0
    parts = [field[0] * field[0] - trace, field[1] * field[1] - trace, field[2] * field[2] - trace,
             field[0] * field[1], field[0] * field[2], field[1] * field[2]]
    return jnp.stack(parts, 0).astype(jnp.bfloat16)


def far_terms(stress, wave_j, axis_one, axis_two, axis_three, y_pos, z_pos):
    points = stress.shape[-1]
    y_count = stress.shape[1]
    z_count = stress.shape[2]
    count = wave_j.shape[0]
    x_pos = jnp.arange(points, dtype=jnp.int32).astype(jnp.float32) * (2.0 * math.pi / points)
    angle_x = wave_j[None, :] * (axis_one[None, :] * x_pos[:, None])
    phase_x = jnp.stack([jnp.cos(angle_x), -jnp.sin(angle_x)], 1).reshape(points, 2 * count).astype(jnp.bfloat16)
    lines = jnp.dot(stress.reshape(6 * y_count * z_count, points), phase_x, preferred_element_type=jnp.float32)
    lines = lines.reshape(6, y_count, z_count, 2, count)
    weights = [axis_one * axis_one, axis_two * axis_two, axis_three * axis_three,
               2.0 * axis_one * axis_two, 2.0 * axis_one * axis_three, 2.0 * axis_two * axis_three]
    mixed = weights[0][None, None, None, :] * lines[0]
    for index in range(1, 6):
        mixed = mixed + weights[index][None, None, None, :] * lines[index]
    angle = wave_j[None, None, :] * (axis_two[None, None, :] * y_pos[:, None, None]) + wave_j[None, None, :] * (axis_three[None, None, :] * z_pos[None, :, None])
    cosine = jnp.cos(angle)
    sine = jnp.sin(angle)
    real_part = mixed[:, :, 0, :]
    imag_part = mixed[:, :, 1, :]
    return jnp.stack([jnp.sum(real_part * cosine + imag_part * sine, (0, 1)),
                      jnp.sum(imag_part * cosine - real_part * sine, (0, 1))], 0)


def reference(velocity_modes, wavenumbers, polar, azimuth):
    table = complex_table(M, N)
    table_x = half_table(KX, N)
    modes = velocity_modes.reshape(3, KX, M, 2, M)

    def along_z(component):
        return jnp.einsum("abpk,pkqz->azqb", component.astype(jnp.float32), table.astype(jnp.float32)).astype(jnp.bfloat16)

    first = lax.map(along_z, modes)

    def along_y(component):
        return jnp.einsum("azpb,pbqy->yzqa", component.astype(jnp.float32), table.astype(jnp.float32)).astype(jnp.bfloat16)

    second = lax.map(along_y, first)
    dirs = polar.shape[0]
    wave_j = jnp.repeat(wavenumbers, dirs)
    axis_one = jnp.tile(jnp.sin(polar) * jnp.cos(azimuth), FREQS)
    axis_two = jnp.tile(jnp.sin(polar) * jnp.sin(azimuth), FREQS)
    axis_three = jnp.tile(jnp.cos(polar), FREQS)
    block = 8
    z_pos = jnp.arange(N, dtype=jnp.int32).astype(jnp.float32) * (2.0 * math.pi / N)

    def one_block(number):
        start = (number * block).astype(jnp.int32)
        piece = lax.dynamic_slice_in_dim(second, start, block, 1)
        field = jnp.einsum("cyzpa,pax->cyzx", piece.astype(jnp.float32), table_x.astype(jnp.float32))
        stress = stresses(field)
        y_pos = (start + jnp.arange(block, dtype=jnp.int32)).astype(jnp.float32) * (2.0 * math.pi / N)
        terms = far_terms(stress, wave_j, axis_one, axis_two, axis_three, y_pos, z_pos)
        return field.astype(jnp.bfloat16), terms

    blocks, terms = lax.map(one_block, jnp.arange(N // block, dtype=jnp.int32))
    velocity = jnp.transpose(blocks, (1, 0, 2, 3, 4)).reshape(3, N, N, N)
    spectrum = jnp.sum(terms, 0).reshape(2, FREQS, dirs)
    spectrum = spectrum * (wavenumbers * wavenumbers)[None, :, None] / (N ** 1.5)
    far_field = jnp.transpose(spectrum, (2, 0, 1))
    return velocity, far_field
```

```python
import functools
import math

import jax
import jax.numpy as jnp
import numpy as np
from jax import lax
from jax.experimental import pallas as pl
from jax.experimental.pallas import tpu as pltpu
from jax.sharding import PartitionSpec as P

N = 512
M = 352
KX = 176
FREQS = 8
DIRS = 32
ROWS = 16
COLS = 32
KL = 11
BF = jnp.bfloat16
F32 = jnp.float32
MESH = pl.DeviceIdType.MESH
NT = (((1,), (1,)), ((), ()))


def tables():
    cos = np.cos(2.0 * np.pi / N * np.arange(N))
    sin = np.sin(2.0 * np.pi / N * np.arange(N))
    waves = np.arange(M) - M // 2
    grid = (waves[None, :] * np.arange(N)[:, None]) % N
    base = np.stack([cos[grid], sin[grid]], 0).reshape(2, COLS, N // COLS, M)
    one = np.zeros((COLS, 2, N // COLS, 384), np.float32)
    one[..., :M] = base.transpose(1, 0, 2, 3)
    one = one.reshape(2 * N, 384)
    grid = (waves[:, None] * np.arange(N)[None, :]) % N
    base = np.stack([cos[grid], -sin[grid]], 0)
    base = base.reshape(2, COLS, KL, ROWS, 4, 8).transpose(1, 0, 2, 4, 5, 3)
    two = np.zeros((COLS, 2, 16, N), np.float32)
    two[:, :, :KL] = base.reshape(COLS, 2, KL, N)
    two = two.reshape(COLS * 32, N)
    half = np.arange(KX)
    grid = (half[:, None] * np.arange(N)[None, :]) % N
    factor = np.where(half == 0, 1.0, 2.0)[:, None]
    base = np.stack([cos[grid], -sin[grid]], 0).astype(jnp.bfloat16).astype(np.float64) * factor
    three = np.zeros((2, ROWS, 16, N), np.float32)
    three[:, :, :KL] = base.reshape(2, ROWS, KL, N)
    three = three.reshape(2 * ROWS * 16, N)
    return [t.astype(jnp.bfloat16) for t in (one, two, three)]


def iota(shape, dim):
    return lax.broadcasted_iota(jnp.int32, shape, dim)


def chosen(condition):
    return jnp.where(condition, 1.0, 0.0)


def swapped(tiles):
    lane = iota((16, 128), 1)
    tiles = list(tiles)
    for bit in range(4):
        step = 1 << bit
        low = (lane & step) == 0
        for i in range(16):
            if i & step:
                continue
            a, b = tiles[i], tiles[i + step]
            tiles[i] = jnp.where(low, a, pltpu.roll(b, step, 1))
            tiles[i + step] = jnp.where(low, pltpu.roll(a, 128 - step, 1), b)
    return tiles


def col_peer(col, i):
    across = lax.rem(i + 1, 2)
    m = i // 2
    shift = jnp.where(m == 0, 8, jnp.where(lax.rem(m, 2) == 1, 8 - (m + 1) // 2, 8 + m // 2))
    x_lo = lax.rem(col // 16 + across, 2)
    return x_lo * 16 + lax.rem(lax.rem(col, 16) + shift, 16)


def kernel(
    modes_hbm, waves_ref, polar_ref, azimuth_ref, one_hbm, two_hbm, three_hbm,
    vel_hbm, far_ref,
    modes, padded, one, two, three, picked_re, picked_im, sent, got, lhs, mid,
    rsent, rgot, lhs_x, field, vel, phase, cos_yz, sin_yz, weights, mixed,
    fsent, fgot, gsent, ggot,
    load_sem, csend, crecv, rsend, rrecv, out_sem, fsend_sem, frecv_sem, gsend_sem, grecv_sem,
):
    row = lax.axis_index("row")
    col = lax.axis_index("col")

    barrier = pltpu.get_barrier_semaphore()

    def greet_col(i, carry):
        pl.semaphore_signal(barrier, inc=1, device_id=(row, col_peer(col, i)), device_id_type=MESH)
        return carry

    def greet_row(i, carry):
        pl.semaphore_signal(
            barrier, inc=1, device_id=(lax.rem(row + i, ROWS), col), device_id_type=MESH
        )
        return carry

    lax.fori_loop(0, COLS - 1, greet_col, 0)
    lax.fori_loop(1, ROWS, greet_row, 0)

    loads = [
        pltpu.make_async_copy(modes_hbm, modes, load_sem.at[0]),
        pltpu.make_async_copy(one_hbm, one, load_sem.at[1]),
        pltpu.make_async_copy(two_hbm, two.at[:, pl.ds(0, N)], load_sem.at[2]),
        pltpu.make_async_copy(three_hbm, three, load_sem.at[3]),
    ]
    for load in loads:
        load.start()

    padded[...] = jnp.zeros_like(padded)
    i, j = iota((128, 176), 0), iota((128, 176), 1)
    pick = chosen((i == (j // 16) * KL + lax.rem(j, 16)) & (lax.rem(j, 16) < KL)).astype(BF)
    loads[0].wait()
    for c in range(3):
        for a in range(KL):
            padded[c, a * 16 : a * 16 + KL, 0 : 2 * M] = modes[c, a]
    for c in range(3):
        rows = jnp.dot(pick, padded[c], preferred_element_type=F32)
        picked_re[c * 128 : (c + 1) * 128, :] = rows[:, :384].astype(BF)
        moved = pltpu.roll(rows, 768 - M, 1)
        picked_im[c * 128 : (c + 1) * 128, :] = moved[:, :384].astype(BF)

    loads[1].wait()

    def along_z(b, carry):
        part = one[pl.ds(pl.multiple_of(b * 256, 256), 256), :]
        pieces = []
        for g in range(8):
            pieces.append(-part[g * 32 + 16 : g * 32 + 32])
            pieces.append(part[g * 32 : g * 32 + 16])
        other = jnp.concatenate(pieces, 0)
        x = lax.dot_general(part, picked_re[...], NT, preferred_element_type=F32)
        x = x + lax.dot_general(other, picked_im[...], NT, preferred_element_type=F32)
        x = x.astype(BF)
        for c in range(3):
            sent[c, pl.ds(b * 8, 8)] = x[:, c * 128 : (c + 1) * 128].reshape(8, 32, 128)
        return carry

    lax.fori_loop(0, 4, along_z, 0)

    pl.semaphore_wait(barrier, COLS + ROWS - 2)

    def send_col(n, carry):
        c = n // (COLS - 1)
        peer = col_peer(col, lax.rem(n, COLS - 1))
        pltpu.make_async_remote_copy(
            src_ref=sent.at[c, peer], dst_ref=got.at[c, col], send_sem=csend.at[c], recv_sem=crecv.at[c],
            device_id=(row, peer), device_id_type=MESH,
        ).start()
        return carry

    lax.fori_loop(0, 3 * (COLS - 1), send_col, 0)
    for c in range(3):
        got[c, pl.ds(col, 1)] = sent[c, pl.ds(col, 1)]

    loads[2].wait()

    def fill_two(b, carry):
        base = pl.multiple_of(b * 32, 32)
        two[pl.ds(base, 16), N : 2 * N] = -two[pl.ds(base + 16, 16), 0:N]
        two[pl.ds(base + 16, 16), N : 2 * N] = two[pl.ds(base, 16), 0:N]
        return carry

    lax.fori_loop(0, COLS, fill_two, 0)

    lane = iota((8, 256), 1)
    wave = jnp.zeros((8, 256), F32)
    polar = jnp.zeros((8, 256), F32)
    azimuth = jnp.zeros((8, 256), F32)
    for m in range(FREQS):
        wave = jnp.where(lane // DIRS == m, waves_ref[m], wave)
    for d in range(DIRS):
        polar = jnp.where(lax.rem(lane, DIRS) == d, polar_ref[d], polar)
        azimuth = jnp.where(lax.rem(lane, DIRS) == d, azimuth_ref[d], azimuth)
    sin_polar = jnp.sin(polar)
    n1 = sin_polar * jnp.cos(azimuth)
    n2 = sin_polar * jnp.sin(azimuth)
    n3 = jnp.cos(polar)
    axes = (n1, n2, n3)
    third = (n1 * n1 + n2 * n2 + n3 * n3) / 3.0
    for c in range(3):
        for e in range(c + 1):
            w = axes[c] * axes[c] - third if e == c else 2.0 * axes[e] * axes[c]
            weights[c, e, :, 0:256] = w
            weights[c, e, :, 256:512] = w
    unit = 2.0 * math.pi / N
    wave_1, one_1, two_1, three_1 = wave[0:1], n1[0:1], n2[0:1], n3[0:1]

    def phases(b, carry):
        base = pl.multiple_of(b * 32, 32)
        index = iota((32, 256), 0) + base
        angle = wave_1 * (one_1 * (index.astype(F32) * unit))
        phase[pl.ds(base, 32), 0:256] = jnp.cos(angle).astype(BF)
        phase[pl.ds(base, 32), 256:512] = (-jnp.sin(angle)).astype(BF)
        y_pos = (row * 32 + index // 16).astype(F32) * unit
        z_pos = (col * 16 + lax.rem(index, 16)).astype(F32) * unit
        angle = wave_1 * (two_1 * y_pos) + wave_1 * (three_1 * z_pos)
        cos_yz[pl.ds(base, 32), :] = jnp.cos(angle)
        sin_yz[pl.ds(base, 32), :] = jnp.sin(angle)
        return carry

    lax.fori_loop(0, 16, phases, 0)
    mixed[...] = jnp.zeros_like(mixed)

    i, j = iota((176, 128), 0), iota((176, 128), 1)
    spread = chosen((j == lax.rem(i, 16) * KL + i // 16) & (lax.rem(i, 16) < KL)).astype(BF)
    turn = chosen(iota((128, 128), 0) == iota((128, 128), 1)).astype(BF)
    loads[3].wait()

    def step(c, carry):
        @pl.when(c < 3)
        def _():
            pltpu.make_async_copy(
                got.at[c, pl.ds(0, COLS - 1)], got.at[c, pl.ds(0, COLS - 1)], crecv.at[c]
            ).wait()
            def regroup(t, carry):
                lines = got[c, pl.ds(t * 4, 4)].reshape(128, 128)
                turned = lax.dot_general(spread, lines, NT, preferred_element_type=F32)
                zero = jnp.zeros((16, 128), F32)
                tiles = [turned[k * 16 : k * 16 + 16] for k in range(KL)] + [zero] * (16 - KL)
                for k, tile in enumerate(swapped(tiles)):
                    lhs[t, k * 16 : k * 16 + 16, :] = tile.astype(BF)
                return carry

            lax.fori_loop(0, 8, regroup, 0)
            wide = jnp.concatenate([lhs[t] for t in range(8)], 1)
            out = jnp.dot(wide, two[...], preferred_element_type=F32)
            for t in range(8):
                mid[t] = out[:, t * 128 : (t + 1) * 128].astype(BF)

            def regroup_row(t, carry):
                tiles = [mid[t, k * 16 : k * 16 + 16, :].astype(F32) for k in range(16)]
                for k, tile in enumerate(swapped(tiles)):
                    rsent[c, k, t] = tile.astype(BF)
                return carry

            lax.fori_loop(0, 8, regroup_row, 0)

            def send_row(k, carry):
                peer = lax.rem(row + k, ROWS)
                pltpu.make_async_remote_copy(
                    src_ref=rsent.at[c, peer], dst_ref=rgot.at[c, row],
                    send_sem=rsend.at[c], recv_sem=rrecv.at[c],
                    device_id=(peer, col), device_id_type=MESH,
                ).start()
                return carry

            lax.fori_loop(1, ROWS, send_row, 0)
            rgot[c, pl.ds(row, 1)] = rsent[c, pl.ds(row, 1)]

        @pl.when(c > 0)
        def _():
            e = c - 1
            pltpu.make_async_copy(
                rgot.at[e, pl.ds(0, ROWS - 1)], rgot.at[e, pl.ds(0, ROWS - 1)], rrecv.at[e]
            ).wait()
            for h in range(4):
                for p in range(2):
                    block = rgot[e, :, p * 4 + h].reshape(256, 128)
                    turned = lax.dot_general(turn, block, NT, preferred_element_type=F32)
                    lhs_x[h * 128 : (h + 1) * 128, p * 256 : (p + 1) * 256] = turned.astype(BF)
            field[e] = jnp.dot(lhs_x[...], three[...], preferred_element_type=F32)
            vel[e] = field[e].astype(BF)
            pltpu.make_async_copy(vel.at[e], vel_hbm.at[e], out_sem.at[e]).start()

            def component(g, carry):
                stress = (field[e] * field[g]).astype(BF)
                lines = jnp.dot(stress, phase[...], preferred_element_type=F32)
                mixed[...] += weights[e, g, 0:1, :] * lines
                return carry

            lax.fori_loop(0, e + 1, component, 0)

        return carry

    lax.fori_loop(0, 4, step, 0)

    re, im = mixed[:, 0:256], mixed[:, 256:512]
    cosine, sine = cos_yz[...], sin_yz[...]
    sum_re = jnp.sum(re * cosine + im * sine, axis=0, keepdims=True)
    sum_im = jnp.sum(im * cosine - re * sine, axis=0, keepdims=True)
    mine = lax.rem(iota((DIRS, 256), 1), DIRS) == iota((DIRS, 256), 0)
    i, j = iota((256, 128), 0) // DIRS, iota((256, 128), 1)
    dot = functools.partial(jnp.dot, preferred_element_type=F32, precision=lax.Precision.HIGHEST)
    per_dir = dot(jnp.where(mine, sum_re, 0.0), chosen(i == j))
    per_dir = per_dir + dot(jnp.where(mine, sum_im, 0.0), chosen(i + FREQS == j))
    for d in range(DIRS):
        fsent[d] = per_dir[d : d + 1]

    def send_far(k, carry):
        peer = col_peer(col, k)
        pltpu.make_async_remote_copy(
            src_ref=fsent.at[peer], dst_ref=fgot.at[col], send_sem=fsend_sem, recv_sem=frecv_sem,
            device_id=(row, peer), device_id_type=MESH,
        ).start()
        return carry

    lax.fori_loop(0, COLS - 1, send_far, 0)
    fgot[pl.ds(col, 1)] = fsent[pl.ds(col, 1)]
    pltpu.make_async_copy(
        fgot.at[pl.ds(0, COLS - 1)], fgot.at[pl.ds(0, COLS - 1)], frecv_sem
    ).wait()
    gsent[...] = jnp.sum(fgot[...], axis=0)

    def send_all(k, carry):
        peer = lax.rem(row + k, ROWS)
        pltpu.make_async_remote_copy(
            src_ref=gsent, dst_ref=ggot.at[row], send_sem=gsend_sem, recv_sem=grecv_sem,
            device_id=(peer, col), device_id_type=MESH,
        ).start()
        return carry

    lax.fori_loop(1, ROWS, send_all, 0)
    ggot[pl.ds(row, 1)] = gsent[...][None]
    pltpu.make_async_copy(
        ggot.at[pl.ds(0, ROWS - 1)], ggot.at[pl.ds(0, ROWS - 1)], grecv_sem
    ).wait()
    total = jnp.sum(ggot[...], axis=0)
    lane = iota((1, 128), 1)
    wave = jnp.zeros((1, 128), F32)
    for m in range(FREQS):
        wave = jnp.where(lax.rem(lane, FREQS) == m, waves_ref[m], wave)
    total = total * (wave * wave) / N**1.5
    far_ref[0, 0:1, :] = total[:, 0:FREQS]
    far_ref[0, 1:2, :] = total[:, FREQS : 2 * FREQS]

    for c in range(3):
        pltpu.make_async_copy(
            sent.at[c, pl.ds(0, COLS - 1)], sent.at[c, pl.ds(0, COLS - 1)], csend.at[c]
        ).wait()
        pltpu.make_async_copy(
            rsent.at[c, pl.ds(0, ROWS - 1)], rsent.at[c, pl.ds(0, ROWS - 1)], rsend.at[c]
        ).wait()
        pltpu.make_async_copy(vel.at[c], vel_hbm.at[c], out_sem.at[c]).wait()
    pltpu.make_async_copy(
        fsent.at[pl.ds(0, COLS - 1)], fsent.at[pl.ds(0, COLS - 1)], fsend_sem
    ).wait()
    pltpu.make_async_copy(
        ggot.at[pl.ds(0, ROWS - 1)], ggot.at[pl.ds(0, ROWS - 1)], gsend_sem
    ).wait()


def body(velocity_modes, wavenumbers, polar, azimuth):
    one, two, three = tables()
    any_space = pl.BlockSpec(memory_space=pl.ANY)
    scalars = pl.BlockSpec(memory_space=pltpu.SMEM)
    dma = pltpu.SemaphoreType.DMA
    velocity, far = pl.pallas_call(
        kernel,
        out_shape=(
            jax.ShapeDtypeStruct((3, N, N), BF),
            jax.ShapeDtypeStruct((1, 2, FREQS), F32),
        ),
        in_specs=[any_space, scalars, scalars, scalars, any_space, any_space, any_space],
        out_specs=(any_space, pl.BlockSpec(memory_space=pltpu.VMEM)),
        scratch_shapes=[
            pltpu.VMEM((3, KL, KL, 2 * M), BF),
            pltpu.VMEM((3, 176, 768), BF),
            pltpu.VMEM((2 * N, 384), BF),
            pltpu.VMEM((2 * N, 2 * N), BF),
            pltpu.VMEM((N, N), BF),
            pltpu.VMEM((384, 384), BF),
            pltpu.VMEM((384, 384), BF),
            pltpu.VMEM((3, COLS, 32, 128), BF),
            pltpu.VMEM((3, COLS, 32, 128), BF),
            pltpu.VMEM((8, 256, 128), BF),
            pltpu.VMEM((8, 256, 128), BF),
            pltpu.VMEM((3, ROWS, 8, 16, 128), BF),
            pltpu.VMEM((3, ROWS, 8, 16, 128), BF),
            pltpu.VMEM((N, N), BF),
            pltpu.VMEM((3, N, N), F32),
            pltpu.VMEM((3, N, N), BF),
            pltpu.VMEM((N, N), BF),
            pltpu.VMEM((N, 256), F32),
            pltpu.VMEM((N, 256), F32),
            pltpu.VMEM((3, 3, 8, N), F32),
            pltpu.VMEM((N, N), F32),
            pltpu.VMEM((COLS, 1, 128), F32),
            pltpu.VMEM((COLS, 1, 128), F32),
            pltpu.VMEM((1, 128), F32),
            pltpu.VMEM((ROWS, 1, 128), F32),
            dma((4,)),
            dma((3,)),
            dma((3,)),
            dma((3,)),
            dma((3,)),
            dma((3,)),
            dma,
            dma,
            dma,
            dma,
        ],
        compiler_params=pltpu.CompilerParams(
            collective_id=0, has_side_effects=True, vmem_limit_bytes=48 * 1024 * 1024
        ),
    )(velocity_modes, wavenumbers, polar, azimuth, jnp.asarray(one), jnp.asarray(two), jnp.asarray(three))
    return velocity.reshape(3, N // ROWS, N // COLS, N), far


def solution(mesh):
    in_specs = (P(None, "row", "col", None), P(), P(), P())
    out_specs = (P(None, "row", "col", None), P("col", None, None))
    return jax.shard_map(body, mesh=mesh, in_specs=in_specs, out_specs=out_specs, check_vma=False)
```

```python
import functools
import math

import jax
import jax.numpy as jnp
import numpy as np
from jax import lax
from jax.experimental import pallas as pl
from jax.experimental.pallas import tpu as pltpu
from jax.sharding import PartitionSpec as P

N = 512
M = 352
KX = 176
FREQS = 8
DIRS = 32
ROWS = 16
COLS = 32
KL = 11
BF = jnp.bfloat16
F32 = jnp.float32
MESH = pl.DeviceIdType.MESH
NT = (((1,), (1,)), ((), ()))


def tables():
    cos = np.cos(2.0 * np.pi / N * np.arange(N))
    sin = np.sin(2.0 * np.pi / N * np.arange(N))
    waves = np.arange(M) - M // 2
    grid = (waves[None, :] * np.arange(N)[:, None]) % N
    base = np.stack([cos[grid], sin[grid]], 0).reshape(2, COLS, 2, 8, M)
    one = np.zeros((2, 2, COLS, 8, 384), np.float32)
    one[..., :M] = base.transpose(0, 2, 1, 3, 4)
    one = one.reshape(2, N, 384)
    grid = (waves[:, None] * np.arange(N)[None, :]) % N
    base = np.zeros((2, COLS, 16, N))
    base[:, :, :KL] = np.stack([cos[grid], -sin[grid]], 0).reshape(2, COLS, KL, N)
    two = base.reshape(2, COLS, 2, 8, 2, 8, 2, 16).transpose(2, 1, 0, 3, 4, 6, 7, 5).reshape(2 * N, N)
    half = np.arange(KX)
    grid = (half[:, None] * np.arange(N)[None, :]) % N
    factor = np.where(half == 0, 1.0, 2.0)[:, None]
    base = np.stack([cos[grid], -sin[grid]], 0).astype(jnp.bfloat16).astype(np.float64) * factor
    three = np.zeros((2, ROWS, 16, N), np.float32)
    three[:, :, :KL] = base.reshape(2, ROWS, KL, N)
    three = three.reshape(2 * ROWS * 16, N)
    return [t.astype(jnp.bfloat16) for t in (one, two, three)]


def iota(shape, dim):
    return lax.broadcasted_iota(jnp.int32, shape, dim)


def chosen(condition):
    return jnp.where(condition, 1.0, 0.0)


def swapped(tiles):
    lane = iota((16, 128), 1)
    tiles = list(tiles)
    for bit in range(3):
        step = 1 << bit
        low = lax.rem(lane // step, 2) == 0
        for i in range(8):
            if (i // step) % 2:
                continue
            a, b = tiles[i], tiles[i + step]
            tiles[i] = jnp.where(low, a, pltpu.roll(b, step, 1))
            tiles[i + step] = jnp.where(low, pltpu.roll(a, 128 - step, 1), b)
    return tiles


SHIFTS = (8, 7, 9, 6, 10, 5, 11, 4, 12, 3, 13, 2, 14, 1, 15, 0)


def col_peers(col):
    base = lax.div(col, 16) * 16
    z = col - base
    peers = []
    for shift in SHIFTS:
        there = lax.rem(z + shift, 16)
        peers.append((16 - base) + there)
        if shift:
            peers.append(base + there)
    return peers


def kernel(
    modes_hbm, waves_hbm, polar_hbm, azimuth_hbm, one_hbm, two_hbm, three_hbm,
    vel_hbm, far_ref,
    waves_ref, polar_ref, azimuth_ref,
    modes, padded, one, two, three, picked_re, picked_im, sent, got, lhs, mid,
    rsent, rgot, lhs_x, field, vel, phase, cos_yz, sin_yz, weights, mixed, spectrum,
    fsent, fgot, gsent, ggot,
    load_sem, csend, crecv, rsend, rrecv, out_sem, fsend_sem, frecv_sem, gsend_sem, grecv_sem,
):
    row = lax.axis_index("row")
    col = lax.axis_index("col")
    peers = col_peers(col)
    row_peers = [lax.rem(row + k, ROWS) for k in range(1, ROWS)]

    barrier = pltpu.get_barrier_semaphore()
    for peer in peers:
        pl.semaphore_signal(barrier, inc=1, device_id=(row, peer), device_id_type=MESH)
    for peer in row_peers:
        pl.semaphore_signal(barrier, inc=1, device_id=(peer, col), device_id_type=MESH)

    loads = [
        pltpu.make_async_copy(modes_hbm, modes, load_sem.at[0]),
        pltpu.make_async_copy(one_hbm, one, load_sem.at[1]),
        pltpu.make_async_copy(two_hbm, two.at[:, pl.ds(0, N)], load_sem.at[2]),
        pltpu.make_async_copy(three_hbm, three, load_sem.at[3]),
        pltpu.make_async_copy(waves_hbm, waves_ref, load_sem.at[4]),
        pltpu.make_async_copy(polar_hbm, polar_ref, load_sem.at[5]),
        pltpu.make_async_copy(azimuth_hbm, azimuth_ref, load_sem.at[6]),
    ]
    for load in loads:
        load.start()

    padded[...] = jnp.zeros_like(padded)
    i, j = iota((384, 488), 0), iota((384, 488), 1)
    pick = chosen((j // 4 == lax.rem(i, 128)) & (lax.rem(j, 4) == i // 128) & (j < 4 * KL * KL)).astype(BF)
    loads[0].wait()
    for a in range(KL):
        for b in range(KL):
            k = (a * KL + b) * 4
            padded[k : k + 3, 0 : 2 * M] = modes[a, b].astype(F32)
    rows = jnp.dot(pick, padded[...].astype(BF), preferred_element_type=F32)
    picked_re[...] = rows[:, :384].astype(BF)
    moved = pltpu.roll(rows, 768 - M, 1)
    picked_im[...] = moved[:, :384].astype(BF)

    loads[1].wait()
    nt = functools.partial(lax.dot_general, dimension_numbers=NT, preferred_element_type=F32)

    def along_z(h, carry):
        cosine = one[0, pl.ds(h * 256, 256), :]
        sine = one[1, pl.ds(h * 256, 256), :]
        x_re = nt(cosine, picked_re[...]) - nt(sine, picked_im[...])
        x_im = nt(sine, picked_re[...]) + nt(cosine, picked_im[...])
        x = jnp.concatenate([x_re.reshape(COLS, 8, 384), x_im.reshape(COLS, 8, 384)], 1).astype(BF)
        for c in range(3):
            sent[h * 3 + c] = x[:, :, c * 128 : (c + 1) * 128]

        @pl.when(h == 0)
        def _():
            pl.semaphore_wait(barrier, COLS + ROWS - 2)

        def send_col(c, carry):
            n = h * 3 + c
            for peer in peers:
                pltpu.make_async_remote_copy(
                    src_ref=sent.at[n, peer], dst_ref=got.at[n, col],
                    send_sem=csend.at[n], recv_sem=crecv.at[n],
                    device_id=(row, peer), device_id_type=MESH,
                ).start()
            got[n, pl.ds(col, 1)] = sent[n, pl.ds(col, 1)]
            return carry

        lax.fori_loop(0, 3, send_col, 0)
        return carry

    lax.fori_loop(0, 2, along_z, 0)

    loads[2].wait()

    def fill_two(b, carry):
        base = pl.multiple_of(b * 64, 64)
        half = two[pl.ds(base, 64), 0:N].astype(F32).reshape(4, 2, 8, N)
        other = jnp.concatenate([-half[:, 1:2], half[:, 0:1]], 1)
        two[pl.ds(base, 64), N : 2 * N] = other.reshape(64, N).astype(BF)
        return carry

    lax.fori_loop(0, 16, fill_two, 0)
    for load in loads[4:]:
        load.wait()

    lane = iota((8, 256), 1)
    wave = jnp.zeros((8, 256), F32)
    polar = jnp.zeros((8, 256), F32)
    azimuth = jnp.zeros((8, 256), F32)
    for m in range(FREQS):
        wave = jnp.where(lane // DIRS == m, waves_ref[m], wave)
    for d in range(DIRS):
        polar = jnp.where(lax.rem(lane, DIRS) == d, polar_ref[d], polar)
        azimuth = jnp.where(lax.rem(lane, DIRS) == d, azimuth_ref[d], azimuth)
    sin_polar = jnp.sin(polar)
    n1 = sin_polar * jnp.cos(azimuth)
    n2 = sin_polar * jnp.sin(azimuth)
    n3 = jnp.cos(polar)
    axes = (n1, n2, n3)
    third = (n1 * n1 + n2 * n2 + n3 * n3) / 3.0
    for c in range(3):
        for e in range(c + 1):
            w = axes[c] * axes[c] - third if e == c else 2.0 * axes[e] * axes[c]
            weights[c, e, :, 0:256] = w
            weights[c, e, :, 256:512] = w
    unit = 2.0 * math.pi / N
    wave_1, one_1, two_1, three_1 = wave[0:1], n1[0:1], n2[0:1], n3[0:1]

    def phases(b, carry):
        base = pl.multiple_of(b * 32, 32)
        index = iota((32, 256), 0) + base
        angle = wave_1 * (one_1 * (index.astype(F32) * unit))
        phase[pl.ds(base, 32), 0:256] = jnp.cos(angle).astype(BF)
        phase[pl.ds(base, 32), 256:512] = (-jnp.sin(angle)).astype(BF)
        part = lax.rem(index, 256)
        y_pos = (row * 32 + part // 8).astype(F32) * unit
        z_pos = (col * 16 + (index // 256) * 8 + lax.rem(part, 8)).astype(F32) * unit
        angle = wave_1 * (two_1 * y_pos) + wave_1 * (three_1 * z_pos)
        cos_yz[pl.ds(base, 32), :] = jnp.cos(angle)
        sin_yz[pl.ds(base, 32), :] = jnp.sin(angle)
        return carry

    lax.fori_loop(0, 16, phases, 0)
    mixed[...] = jnp.zeros_like(mixed)
    spectrum[...] = jnp.zeros_like(spectrum)

    i, j = iota((176, 128), 0), iota((176, 128), 1)
    spread = chosen((j == lax.rem(i, 16) * KL + i // 16) & (lax.rem(i, 16) < KL)).astype(BF)
    turn = chosen(iota((128, 128), 0) == iota((128, 128), 1)).astype(BF)
    loads[3].wait()

    def step(n, carry):
        @pl.when(n < 6)
        def _():
            pltpu.make_async_copy(
                got.at[n, pl.ds(0, COLS - 1)], got.at[n, pl.ds(0, COLS - 1)], crecv.at[n]
            ).wait()

            def regroup(pair, carry):
                for k in range(2):
                    t = pair * 2 + k
                    lines = got[n, pl.ds(t * 8, 8)].reshape(128, 128)
                    turned = nt(spread, lines).astype(BF)
                    zero = jnp.zeros((16, 128), BF)
                    tiles = [turned[m * 16 : m * 16 + 16] for m in range(KL)] + [zero] * (16 - KL)
                    for m, tile in enumerate(swapped(tiles[:8])):
                        lhs[t, m * 16 : m * 16 + 16, :] = tile
                    for m, tile in enumerate(swapped(tiles[8:])):
                        lhs[t + 4, m * 16 : m * 16 + 16, :] = tile
                return carry

            lax.fori_loop(0, 2, regroup, 0)
            wide = jnp.concatenate([lhs[t] for t in range(8)], 1)
            out = jnp.dot(wide, two[...], preferred_element_type=F32)
            for t in range(8):
                mid[t] = out[:, t * 128 : (t + 1) * 128].astype(BF)

            def regroup_row(part, carry):
                for upper in range(2):
                    for y_upper in range(2):
                        t = part * 4 + upper * 2 + y_upper
                        tiles = [mid[t, k * 16 : k * 16 + 16, :] for k in range(8)]
                        for k, tile in enumerate(swapped(tiles)):
                            rsent[n, upper * 8 + k, part * 2 + y_upper] = tile
                return carry

            lax.fori_loop(0, 2, regroup_row, 0)
            for peer in row_peers:
                pltpu.make_async_remote_copy(
                    src_ref=rsent.at[n, peer], dst_ref=rgot.at[n, row],
                    send_sem=rsend.at[n], recv_sem=rrecv.at[n],
                    device_id=(peer, col), device_id_type=MESH,
                ).start()
            rgot[n, pl.ds(row, 1)] = rsent[n, pl.ds(row, 1)]

        @pl.when(n > 0)
        def _():
            e = n - 1
            h = lax.div(e, 3)
            c = e - 3 * h
            pltpu.make_async_copy(
                rgot.at[e, pl.ds(0, ROWS - 1)], rgot.at[e, pl.ds(0, ROWS - 1)], rrecv.at[e]
            ).wait()
            for y_upper in range(2):
                for p in range(2):
                    block = rgot[e, :, p * 2 + y_upper].reshape(256, 128)
                    lhs_x[y_upper * 128 : (y_upper + 1) * 128, p * 256 : (p + 1) * 256] = nt(turn, block).astype(BF)
            field[c] = jnp.dot(lhs_x[...], three[...], preferred_element_type=F32)
            vel[e] = field[c].reshape(32, 8, N).astype(BF)
            pltpu.make_async_copy(vel.at[e], vel_hbm.at[c, :, pl.ds(h * 8, 8), :], out_sem.at[e]).start()

            def component(g, carry):
                stress = (field[c] * field[g]).astype(BF)
                lines = jnp.dot(stress, phase[...], preferred_element_type=F32)
                mixed[...] += weights[c, g, 0:1, :] * lines
                return carry

            lax.fori_loop(0, c + 1, component, 0)

            @pl.when(c == 2)
            def _():
                re, im = mixed[:, 0:256], mixed[:, 256:512]
                cosine, sine = cos_yz[pl.ds(h * 256, 256), :], sin_yz[pl.ds(h * 256, 256), :]
                spectrum[0:1, :] += jnp.sum(re * cosine + im * sine, axis=0, keepdims=True)
                spectrum[1:2, :] += jnp.sum(im * cosine - re * sine, axis=0, keepdims=True)
                mixed[...] = jnp.zeros_like(mixed)

        return carry

    lax.fori_loop(0, 7, step, 0)

    sum_re, sum_im = spectrum[0:1, :], spectrum[1:2, :]
    mine = lax.rem(iota((DIRS, 256), 1), DIRS) == iota((DIRS, 256), 0)
    i, j = iota((256, 128), 0) // DIRS, iota((256, 128), 1)
    dot = functools.partial(jnp.dot, preferred_element_type=F32, precision=lax.Precision.HIGHEST)
    per_dir = dot(jnp.where(mine, sum_re, 0.0), chosen(i == j))
    per_dir = per_dir + dot(jnp.where(mine, sum_im, 0.0), chosen(i + FREQS == j))
    for d in range(DIRS):
        fsent[d] = per_dir[d : d + 1]

    for peer in peers:
        pltpu.make_async_remote_copy(
            src_ref=fsent.at[peer], dst_ref=fgot.at[col], send_sem=fsend_sem, recv_sem=frecv_sem,
            device_id=(row, peer), device_id_type=MESH,
        ).start()
    fgot[pl.ds(col, 1)] = fsent[pl.ds(col, 1)]
    pltpu.make_async_copy(
        fgot.at[pl.ds(0, COLS - 1)], fgot.at[pl.ds(0, COLS - 1)], frecv_sem
    ).wait()
    gsent[...] = jnp.sum(fgot[...], axis=0)

    for peer in row_peers:
        pltpu.make_async_remote_copy(
            src_ref=gsent, dst_ref=ggot.at[row], send_sem=gsend_sem, recv_sem=grecv_sem,
            device_id=(peer, col), device_id_type=MESH,
        ).start()
    ggot[pl.ds(row, 1)] = gsent[...][None]
    pltpu.make_async_copy(
        ggot.at[pl.ds(0, ROWS - 1)], ggot.at[pl.ds(0, ROWS - 1)], grecv_sem
    ).wait()
    total = jnp.sum(ggot[...], axis=0)
    lane = iota((1, 128), 1)
    wave = jnp.zeros((1, 128), F32)
    for m in range(FREQS):
        wave = jnp.where(lax.rem(lane, FREQS) == m, waves_ref[m], wave)
    total = total * (wave * wave) / N**1.5
    far_ref[0, 0:1, :] = total[:, 0:FREQS]
    far_ref[0, 1:2, :] = total[:, FREQS : 2 * FREQS]

    for c in range(6):
        pltpu.make_async_copy(
            sent.at[c, pl.ds(0, COLS - 1)], sent.at[c, pl.ds(0, COLS - 1)], csend.at[c]
        ).wait()
        pltpu.make_async_copy(
            rsent.at[c, pl.ds(0, ROWS - 1)], rsent.at[c, pl.ds(0, ROWS - 1)], rsend.at[c]
        ).wait()
        pltpu.make_async_copy(vel.at[c], vel_hbm.at[c % 3, :, pl.ds(c // 3 * 8, 8), :], out_sem.at[c]).wait()
    pltpu.make_async_copy(
        fsent.at[pl.ds(0, COLS - 1)], fsent.at[pl.ds(0, COLS - 1)], fsend_sem
    ).wait()
    pltpu.make_async_copy(
        ggot.at[pl.ds(0, ROWS - 1)], ggot.at[pl.ds(0, ROWS - 1)], gsend_sem
    ).wait()


def body(velocity_modes, wavenumbers, polar, azimuth):
    one, two, three = tables()
    hbm = pl.BlockSpec(memory_space=pltpu.HBM)
    dma = pltpu.SemaphoreType.DMA
    return pl.pallas_call(
        kernel,
        out_shape=(
            jax.ShapeDtypeStruct((3, N // ROWS, N // COLS, N), BF),
            jax.ShapeDtypeStruct((1, 2, FREQS), F32),
        ),
        in_specs=[hbm] * 7,
        out_specs=(pl.BlockSpec(memory_space=pl.ANY), pl.BlockSpec(memory_space=pltpu.VMEM)),
        scratch_shapes=[
            pltpu.SMEM((FREQS,), F32),
            pltpu.SMEM((DIRS,), F32),
            pltpu.SMEM((DIRS,), F32),
            pltpu.VMEM((KL, KL, 3, 2 * M), BF),
            pltpu.VMEM((488, 768), F32),
            pltpu.VMEM((2, N, 384), BF),
            pltpu.VMEM((2 * N, 2 * N), BF),
            pltpu.VMEM((N, N), BF),
            pltpu.VMEM((384, 384), BF),
            pltpu.VMEM((384, 384), BF),
            pltpu.VMEM((6, COLS, 16, 128), BF),
            pltpu.VMEM((6, COLS, 16, 128), BF),
            pltpu.VMEM((8, 128, 128), BF),
            pltpu.VMEM((8, 128, 128), BF),
            pltpu.VMEM((6, ROWS, 4, 16, 128), BF),
            pltpu.VMEM((6, ROWS, 4, 16, 128), BF),
            pltpu.VMEM((256, N), BF),
            pltpu.VMEM((3, 256, N), F32),
            pltpu.VMEM((6, 32, 8, N), BF),
            pltpu.VMEM((N, N), BF),
            pltpu.VMEM((N, 256), F32),
            pltpu.VMEM((N, 256), F32),
            pltpu.VMEM((3, 3, 8, N), F32),
            pltpu.VMEM((256, N), F32),
            pltpu.VMEM((8, 256), F32),
            pltpu.VMEM((COLS, 1, 128), F32),
            pltpu.VMEM((COLS, 1, 128), F32),
            pltpu.VMEM((1, 128), F32),
            pltpu.VMEM((ROWS, 1, 128), F32),
            dma((7,)),
            dma((6,)),
            dma((6,)),
            dma((6,)),
            dma((6,)),
            dma((6,)),
            dma,
            dma,
            dma,
            dma,
        ],
        compiler_params=pltpu.CompilerParams(
            collective_id=0, has_side_effects=True, vmem_limit_bytes=67043328
        ),
    )(jnp.transpose(velocity_modes, (1, 2, 0, 3)), wavenumbers, polar, azimuth, jnp.asarray(one), jnp.asarray(two), jnp.asarray(three))


def solution(mesh):
    in_specs = (P(None, "row", "col", None), P(), P(), P())
    out_specs = (P(None, "row", "col", None), P("col", None, None))
    return jax.shard_map(body, mesh=mesh, in_specs=in_specs, out_specs=out_specs, check_vma=False)
```

```python
import functools
import math

import jax
import jax.numpy as jnp
import numpy as np
from jax import lax
from jax.experimental import pallas as pl
from jax.experimental.pallas import tpu as pltpu
from jax.sharding import PartitionSpec as P

N = 512
M = 352
KX = 176
FREQS = 8
DIRS = 32
ROWS = 16
COLS = 32
KL = 11
BF = jnp.bfloat16
F32 = jnp.float32
MESH = pl.DeviceIdType.MESH
NT = (((1,), (1,)), ((), ()))


def tables():
    cos = np.cos(2.0 * np.pi / N * np.arange(N))
    sin = np.sin(2.0 * np.pi / N * np.arange(N))
    waves = np.arange(M) - M // 2
    grid = (waves[None, :] * np.arange(N)[:, None]) % N
    base = np.stack([cos[grid], sin[grid]], 0).reshape(2, COLS, 2, 8, M)
    one = np.zeros((2, 2, COLS, 8, 384), np.float32)
    one[..., :M] = base.transpose(0, 2, 1, 3, 4)
    one = one.reshape(2, N, 384)
    grid = (waves[:, None] * np.arange(N)[None, :]) % N
    base = np.zeros((2, COLS, 16, N))
    base[:, :, :KL] = np.stack([cos[grid], -sin[grid]], 0).reshape(2, COLS, KL, N)
    two = base.reshape(2, COLS, 2, 8, 2, 8, 2, 16).transpose(2, 1, 0, 3, 4, 6, 7, 5).reshape(2 * N, N)
    half = np.arange(KX)
    grid = (half[:, None] * np.arange(N)[None, :]) % N
    factor = np.where(half == 0, 1.0, 2.0)[:, None]
    base = np.stack([cos[grid], -sin[grid]], 0).astype(jnp.bfloat16).astype(np.float64) * factor
    three = np.zeros((2, ROWS, 16, N), np.float32)
    three[:, :, :KL] = base.reshape(2, ROWS, KL, N)
    three = three.reshape(2 * ROWS * 16, N)
    return [t.astype(jnp.bfloat16) for t in (one, two, three)]


def iota(shape, dim):
    return lax.broadcasted_iota(jnp.int32, shape, dim)


def chosen(condition):
    return jnp.where(condition, 1.0, 0.0)


def swapped(tiles):
    lane = iota((16, 128), 1)
    tiles = list(tiles)
    for bit in range(3):
        step = 1 << bit
        low = lax.rem(lane // step, 2) == 0
        for i in range(8):
            if (i // step) % 2:
                continue
            a, b = tiles[i], tiles[i + step]
            tiles[i] = jnp.where(low, a, pltpu.roll(b, step, 1))
            tiles[i + step] = jnp.where(low, pltpu.roll(a, 128 - step, 1), b)
    return tiles


SHIFTS = (8, 7, 9, 6, 10, 5, 11, 4, 12, 3, 13, 2, 14, 1, 15, 0)


def col_peers(col):
    base = lax.div(col, 16) * 16
    z = col - base
    peers = []
    for shift in SHIFTS:
        there = lax.rem(z + shift, 16)
        peers.append((16 - base) + there)
        if shift:
            peers.append(base + there)
    return peers


def kernel(
    modes_hbm, waves_hbm, polar_hbm, azimuth_hbm, one_hbm, two_hbm, three_hbm,
    vel_ref, far_ref,
    waves_ref, polar_ref, azimuth_ref,
    modes, padded, one, two, three, picked_re, picked_im, sent, got, lhs, mid,
    rsent, rgot, lhs_x, field, phase, cos_yz, sin_yz, weights, mixed, spectrum,
    fsent, fgot, gsent, ggot,
    load_sem, csend, crecv, rsend, rrecv, fsend_sem, frecv_sem, gsend_sem, grecv_sem,
):
    row = lax.axis_index("row")
    col = lax.axis_index("col")
    peers = col_peers(col)
    row_peers = [lax.rem(row + k, ROWS) for k in range(1, ROWS)]

    barrier = pltpu.get_barrier_semaphore()
    for peer in peers:
        pl.semaphore_signal(barrier, inc=1, device_id=(row, peer), device_id_type=MESH)
    for peer in row_peers:
        pl.semaphore_signal(barrier, inc=1, device_id=(peer, col), device_id_type=MESH)

    loads = [
        pltpu.make_async_copy(modes_hbm, modes, load_sem.at[0]),
        pltpu.make_async_copy(one_hbm, one, load_sem.at[1]),
        pltpu.make_async_copy(two_hbm, two.at[:, pl.ds(0, N)], load_sem.at[2]),
        pltpu.make_async_copy(three_hbm, three, load_sem.at[3]),
        pltpu.make_async_copy(waves_hbm, waves_ref, load_sem.at[4]),
        pltpu.make_async_copy(polar_hbm, polar_ref, load_sem.at[5]),
        pltpu.make_async_copy(azimuth_hbm, azimuth_ref, load_sem.at[6]),
    ]
    for load in loads:
        load.start()

    padded[...] = jnp.zeros_like(padded)
    i, j = iota((384, 488), 0), iota((384, 488), 1)
    pick = chosen((j // 4 == lax.rem(i, 128)) & (lax.rem(j, 4) == i // 128) & (j < 4 * KL * KL)).astype(BF)
    loads[0].wait()
    for a in range(KL):
        for b in range(KL):
            k = (a * KL + b) * 4
            padded[k : k + 3, 0 : 2 * M] = modes[a, b].astype(F32)
    rows = jnp.dot(pick, padded[...].astype(BF), preferred_element_type=F32)
    picked_re[...] = rows[:, :384].astype(BF)
    moved = pltpu.roll(rows, 768 - M, 1)
    picked_im[...] = moved[:, :384].astype(BF)

    loads[1].wait()
    nt = functools.partial(lax.dot_general, dimension_numbers=NT, preferred_element_type=F32)

    def along_z(h, carry):
        cosine = one[0, pl.ds(h * 256, 256), :]
        sine = one[1, pl.ds(h * 256, 256), :]
        x_re = nt(cosine, picked_re[...]) - nt(sine, picked_im[...])
        x_im = nt(sine, picked_re[...]) + nt(cosine, picked_im[...])
        x = jnp.concatenate([x_re.reshape(COLS, 8, 384), x_im.reshape(COLS, 8, 384)], 1).astype(BF)
        for c in range(3):
            sent[h * 3 + c] = x[:, :, c * 128 : (c + 1) * 128]

        @pl.when(h == 0)
        def _():
            pl.semaphore_wait(barrier, COLS + ROWS - 2)

        def send_col(c, carry):
            n = h * 3 + c
            for peer in peers:
                pltpu.make_async_remote_copy(
                    src_ref=sent.at[n, peer], dst_ref=got.at[n, col],
                    send_sem=csend.at[n], recv_sem=crecv.at[n],
                    device_id=(row, peer), device_id_type=MESH,
                ).start()
            got[n, pl.ds(col, 1)] = sent[n, pl.ds(col, 1)]
            return carry

        lax.fori_loop(0, 3, send_col, 0)
        return carry

    lax.fori_loop(0, 2, along_z, 0)

    loads[2].wait()

    def fill_two(b, carry):
        base = pl.multiple_of(b * 64, 64)
        half = two[pl.ds(base, 64), 0:N].astype(F32).reshape(4, 2, 8, N)
        other = jnp.concatenate([-half[:, 1:2], half[:, 0:1]], 1)
        two[pl.ds(base, 64), N : 2 * N] = other.reshape(64, N).astype(BF)
        return carry

    lax.fori_loop(0, 16, fill_two, 0)
    for load in loads[4:]:
        load.wait()

    lane = iota((8, 256), 1)
    wave = jnp.zeros((8, 256), F32)
    polar = jnp.zeros((8, 256), F32)
    azimuth = jnp.zeros((8, 256), F32)
    for m in range(FREQS):
        wave = jnp.where(lane // DIRS == m, waves_ref[m], wave)
    for d in range(DIRS):
        polar = jnp.where(lax.rem(lane, DIRS) == d, polar_ref[d], polar)
        azimuth = jnp.where(lax.rem(lane, DIRS) == d, azimuth_ref[d], azimuth)
    sin_polar = jnp.sin(polar)
    n1 = sin_polar * jnp.cos(azimuth)
    n2 = sin_polar * jnp.sin(azimuth)
    n3 = jnp.cos(polar)
    axes = (n1, n2, n3)
    third = (n1 * n1 + n2 * n2 + n3 * n3) / 3.0
    for c in range(3):
        for e in range(c + 1):
            w = axes[c] * axes[c] - third if e == c else 2.0 * axes[e] * axes[c]
            weights[c, e, :, 0:256] = w
            weights[c, e, :, 256:512] = w
    unit = 2.0 * math.pi / N
    wave_1, one_1, two_1, three_1 = wave[0:1], n1[0:1], n2[0:1], n3[0:1]

    def phases(b, carry):
        base = pl.multiple_of(b * 32, 32)
        index = iota((32, 256), 0) + base
        angle = wave_1 * (one_1 * (index.astype(F32) * unit))
        phase[pl.ds(base, 32), 0:256] = jnp.cos(angle).astype(BF)
        phase[pl.ds(base, 32), 256:512] = (-jnp.sin(angle)).astype(BF)
        part = lax.rem(index, 256)
        y_pos = (row * 32 + part // 8).astype(F32) * unit
        z_pos = (col * 16 + (index // 256) * 8 + lax.rem(part, 8)).astype(F32) * unit
        angle = wave_1 * (two_1 * y_pos) + wave_1 * (three_1 * z_pos)
        cos_yz[pl.ds(base, 32), :] = jnp.cos(angle)
        sin_yz[pl.ds(base, 32), :] = jnp.sin(angle)
        return carry

    lax.fori_loop(0, 16, phases, 0)
    mixed[...] = jnp.zeros_like(mixed)
    spectrum[...] = jnp.zeros_like(spectrum)

    i, j = iota((176, 128), 0), iota((176, 128), 1)
    spread = chosen((j == lax.rem(i, 16) * KL + i // 16) & (lax.rem(i, 16) < KL)).astype(BF)
    turn = chosen(iota((128, 128), 0) == iota((128, 128), 1)).astype(BF)
    loads[3].wait()

    def step(n, carry):
        @pl.when(n < 6)
        def _():
            pltpu.make_async_copy(
                got.at[n, pl.ds(0, COLS - 1)], got.at[n, pl.ds(0, COLS - 1)], crecv.at[n]
            ).wait()

            def regroup(pair, carry):
                for k in range(2):
                    t = pair * 2 + k
                    lines = got[n, pl.ds(t * 8, 8)].reshape(128, 128)
                    turned = nt(spread, lines).astype(BF)
                    zero = jnp.zeros((16, 128), BF)
                    tiles = [turned[m * 16 : m * 16 + 16] for m in range(KL)] + [zero] * (16 - KL)
                    for m, tile in enumerate(swapped(tiles[:8])):
                        lhs[t, m * 16 : m * 16 + 16, :] = tile
                    for m, tile in enumerate(swapped(tiles[8:])):
                        lhs[t + 4, m * 16 : m * 16 + 16, :] = tile
                return carry

            lax.fori_loop(0, 2, regroup, 0)
            wide = jnp.concatenate([lhs[t] for t in range(8)], 1)
            out = jnp.dot(wide, two[...], preferred_element_type=F32)
            for t in range(8):
                mid[t] = out[:, t * 128 : (t + 1) * 128].astype(BF)

            def regroup_row(part, carry):
                for upper in range(2):
                    for y_upper in range(2):
                        t = part * 4 + upper * 2 + y_upper
                        tiles = [mid[t, k * 16 : k * 16 + 16, :] for k in range(8)]
                        for k, tile in enumerate(swapped(tiles)):
                            rsent[n, upper * 8 + k, part * 2 + y_upper] = tile
                return carry

            lax.fori_loop(0, 2, regroup_row, 0)
            for peer in row_peers:
                pltpu.make_async_remote_copy(
                    src_ref=rsent.at[n, peer], dst_ref=rgot.at[n, row],
                    send_sem=rsend.at[n], recv_sem=rrecv.at[n],
                    device_id=(peer, col), device_id_type=MESH,
                ).start()
            rgot[n, pl.ds(row, 1)] = rsent[n, pl.ds(row, 1)]

        @pl.when(n > 0)
        def _():
            e = n - 1
            h = lax.div(e, 3)
            c = e - 3 * h
            pltpu.make_async_copy(
                rgot.at[e, pl.ds(0, ROWS - 1)], rgot.at[e, pl.ds(0, ROWS - 1)], rrecv.at[e]
            ).wait()
            for y_upper in range(2):
                for p in range(2):
                    block = rgot[e, :, p * 2 + y_upper].reshape(256, 128)
                    lhs_x[y_upper * 128 : (y_upper + 1) * 128, p * 256 : (p + 1) * 256] = nt(turn, block).astype(BF)
            field[c] = jnp.dot(lhs_x[...], three[...], preferred_element_type=F32)
            for k in range(2):

                @pl.when(h == k)
                def _():
                    vel_ref[c, :, k * 8 : k * 8 + 8, :] = field[c].reshape(32, 8, N).astype(BF)

            def component(g, carry):
                stress = (field[c] * field[g]).astype(BF)
                lines = jnp.dot(stress, phase[...], preferred_element_type=F32)
                mixed[...] += weights[c, g, 0:1, :] * lines
                return carry

            lax.fori_loop(0, c + 1, component, 0)

            @pl.when(c == 2)
            def _():
                re, im = mixed[:, 0:256], mixed[:, 256:512]
                cosine, sine = cos_yz[pl.ds(h * 256, 256), :], sin_yz[pl.ds(h * 256, 256), :]
                spectrum[0:1, :] += jnp.sum(re * cosine + im * sine, axis=0, keepdims=True)
                spectrum[1:2, :] += jnp.sum(im * cosine - re * sine, axis=0, keepdims=True)
                mixed[...] = jnp.zeros_like(mixed)

        return carry

    lax.fori_loop(0, 7, step, 0)

    sum_re, sum_im = spectrum[0:1, :], spectrum[1:2, :]
    mine = lax.rem(iota((DIRS, 256), 1), DIRS) == iota((DIRS, 256), 0)
    i, j = iota((256, 128), 0) // DIRS, iota((256, 128), 1)
    dot = functools.partial(jnp.dot, preferred_element_type=F32, precision=lax.Precision.HIGHEST)
    per_dir = dot(jnp.where(mine, sum_re, 0.0), chosen(i == j))
    per_dir = per_dir + dot(jnp.where(mine, sum_im, 0.0), chosen(i + FREQS == j))
    for d in range(DIRS):
        fsent[d] = per_dir[d : d + 1]

    for peer in peers:
        pltpu.make_async_remote_copy(
            src_ref=fsent.at[peer], dst_ref=fgot.at[col], send_sem=fsend_sem, recv_sem=frecv_sem,
            device_id=(row, peer), device_id_type=MESH,
        ).start()
    fgot[pl.ds(col, 1)] = fsent[pl.ds(col, 1)]
    pltpu.make_async_copy(
        fgot.at[pl.ds(0, COLS - 1)], fgot.at[pl.ds(0, COLS - 1)], frecv_sem
    ).wait()
    gsent[...] = jnp.sum(fgot[...], axis=0)

    for peer in row_peers:
        pltpu.make_async_remote_copy(
            src_ref=gsent, dst_ref=ggot.at[row], send_sem=gsend_sem, recv_sem=grecv_sem,
            device_id=(peer, col), device_id_type=MESH,
        ).start()
    ggot[pl.ds(row, 1)] = gsent[...][None]
    pltpu.make_async_copy(
        ggot.at[pl.ds(0, ROWS - 1)], ggot.at[pl.ds(0, ROWS - 1)], grecv_sem
    ).wait()
    total = jnp.sum(ggot[...], axis=0)
    lane = iota((1, 128), 1)
    wave = jnp.zeros((1, 128), F32)
    for m in range(FREQS):
        wave = jnp.where(lax.rem(lane, FREQS) == m, waves_ref[m], wave)
    total = total * (wave * wave) / N**1.5
    far_ref[0, 0:1, :] = total[:, 0:FREQS]
    far_ref[0, 1:2, :] = total[:, FREQS : 2 * FREQS]

    for c in range(6):
        pltpu.make_async_copy(
            sent.at[c, pl.ds(0, COLS - 1)], sent.at[c, pl.ds(0, COLS - 1)], csend.at[c]
        ).wait()
        pltpu.make_async_copy(
            rsent.at[c, pl.ds(0, ROWS - 1)], rsent.at[c, pl.ds(0, ROWS - 1)], rsend.at[c]
        ).wait()
    pltpu.make_async_copy(
        fsent.at[pl.ds(0, COLS - 1)], fsent.at[pl.ds(0, COLS - 1)], fsend_sem
    ).wait()
    pltpu.make_async_copy(
        ggot.at[pl.ds(0, ROWS - 1)], ggot.at[pl.ds(0, ROWS - 1)], gsend_sem
    ).wait()


def body(velocity_modes, wavenumbers, polar, azimuth):
    one, two, three = tables()
    hbm = pl.BlockSpec(memory_space=pltpu.HBM)
    dma = pltpu.SemaphoreType.DMA
    return pl.pallas_call(
        kernel,
        out_shape=(
            pltpu.VMEM((3, N // ROWS, N // COLS, N), BF),
            pltpu.VMEM((1, 2, FREQS), F32),
        ),
        in_specs=[hbm] * 7,
        out_specs=(pl.BlockSpec(memory_space=pltpu.VMEM), pl.BlockSpec(memory_space=pltpu.VMEM)),
        scratch_shapes=[
            pltpu.SMEM((FREQS,), F32),
            pltpu.SMEM((DIRS,), F32),
            pltpu.SMEM((DIRS,), F32),
            pltpu.VMEM((KL, KL, 3, 2 * M), BF),
            pltpu.VMEM((488, 768), F32),
            pltpu.VMEM((2, N, 384), BF),
            pltpu.VMEM((2 * N, 2 * N), BF),
            pltpu.VMEM((N, N), BF),
            pltpu.VMEM((384, 384), BF),
            pltpu.VMEM((384, 384), BF),
            pltpu.VMEM((6, COLS, 16, 128), BF),
            pltpu.VMEM((6, COLS, 16, 128), BF),
            pltpu.VMEM((8, 128, 128), BF),
            pltpu.VMEM((8, 128, 128), BF),
            pltpu.VMEM((6, ROWS, 4, 16, 128), BF),
            pltpu.VMEM((6, ROWS, 4, 16, 128), BF),
            pltpu.VMEM((256, N), BF),
            pltpu.VMEM((3, 256, N), F32),
            pltpu.VMEM((N, N), BF),
            pltpu.VMEM((N, 256), F32),
            pltpu.VMEM((N, 256), F32),
            pltpu.VMEM((3, 3, 8, N), F32),
            pltpu.VMEM((256, N), F32),
            pltpu.VMEM((8, 256), F32),
            pltpu.VMEM((COLS, 1, 128), F32),
            pltpu.VMEM((COLS, 1, 128), F32),
            pltpu.VMEM((1, 128), F32),
            pltpu.VMEM((ROWS, 1, 128), F32),
            dma((7,)),
            dma((6,)),
            dma((6,)),
            dma((6,)),
            dma((6,)),
            dma,
            dma,
            dma,
            dma,
        ],
        compiler_params=pltpu.CompilerParams(
            collective_id=0, has_side_effects=True, vmem_limit_bytes=65000000
        ),
    )(jnp.transpose(velocity_modes, (1, 2, 0, 3)), wavenumbers, polar, azimuth, jnp.asarray(one), jnp.asarray(two), jnp.asarray(three))


def solution(mesh):
    in_specs = (P(None, "row", "col", None), P(), P(), P())
    out_specs = (P(None, "row", "col", None), P("col", None, None))
    return jax.shard_map(body, mesh=mesh, in_specs=in_specs, out_specs=out_specs, check_vma=False)
```

```python
import functools
import math

import jax
import jax.numpy as jnp
import numpy as np
from jax import lax
from jax.experimental import pallas as pl
from jax.experimental.pallas import tpu as pltpu
from jax.sharding import PartitionSpec as P

N = 512
M = 352
KX = 176
FREQS = 8
DIRS = 32
ROWS = 16
COLS = 32
KL = 11
BF = jnp.bfloat16
F32 = jnp.float32
MESH = pl.DeviceIdType.MESH
NT = (((1,), (1,)), ((), ()))


def tables():
    cos = np.cos(2.0 * np.pi / N * np.arange(N))
    sin = np.sin(2.0 * np.pi / N * np.arange(N))
    waves = np.arange(M) - M // 2
    grid = (waves[None, :] * np.arange(N)[:, None]) % N
    base = np.stack([cos[grid], sin[grid]], 0).reshape(2, COLS, 4, 4, M)
    one = np.zeros((4, COLS, 2, 4, 384), np.float32)
    one[..., :M] = base.transpose(2, 1, 0, 3, 4)
    one = one.reshape(2 * N, 384)
    grid = (waves[:, None] * np.arange(N)[None, :]) % N
    base = np.zeros((2, COLS, 12, N))
    base[:, :, :KL] = np.stack([cos[grid], -sin[grid]], 0).reshape(2, COLS, KL, N)
    two = base.reshape(2, COLS, 3, 4, 4, 4, 32).transpose(2, 1, 0, 3, 4, 6, 5).reshape(24 * COLS, N)
    half = np.arange(KX)
    grid = (half[:, None] * np.arange(N)[None, :]) % N
    factor = np.where(half == 0, 1.0, 2.0)[:, None]
    base = np.stack([cos[grid], -sin[grid]], 0).astype(jnp.bfloat16).astype(np.float64) * factor
    three = np.zeros((2, ROWS, 16, N), np.float32)
    three[:, :, :KL] = base.reshape(2, ROWS, KL, N)
    three = three.reshape(2 * ROWS * 16, N)
    return [t.astype(jnp.bfloat16) for t in (one, two, three)]


def iota(shape, dim):
    return lax.broadcasted_iota(jnp.int32, shape, dim)


def chosen(condition):
    return jnp.where(condition, 1.0, 0.0)


def swapped(tiles):
    lane = iota((16, 128), 1)
    tiles = list(tiles)
    for bit in range(2):
        step = 1 << bit
        low = lax.rem(lane // step, 2) == 0
        for i in range(4):
            if (i // step) % 2:
                continue
            a, b = tiles[i], tiles[i + step]
            tiles[i] = jnp.where(low, a, pltpu.roll(b, step, 1))
            tiles[i + step] = jnp.where(low, pltpu.roll(a, 128 - step, 1), b)
    return tiles


SHIFTS = (8, 7, 9, 6, 10, 5, 11, 4, 12, 3, 13, 2, 14, 1, 15, 0)


def col_peers(col):
    base = lax.div(col, 16) * 16
    z = col - base
    peers = []
    for shift in SHIFTS:
        there = lax.rem(z + shift, 16)
        peers.append((16 - base) + there)
        if shift:
            peers.append(base + there)
    return peers


def kernel(
    modes_hbm, waves_hbm, polar_hbm, azimuth_hbm, one_hbm, two_hbm, three_hbm,
    vel_ref, far_ref,
    waves_ref, polar_ref, azimuth_ref,
    modes, padded, one, two, three, picked_re, picked_im, sent, got, lhs, mid,
    rsent, rgot, lhs_x, field, phase, cos_yz, sin_yz, weights, mixed, spectrum,
    fsent, fgot, gsent, ggot,
    load_sem, csend, crecv, rsend, rrecv, fsend_sem, frecv_sem, gsend_sem, grecv_sem,
):
    row = lax.axis_index("row")
    col = lax.axis_index("col")
    peers = col_peers(col)
    row_peers = [lax.rem(row + k, ROWS) for k in range(1, ROWS)]

    barrier = pltpu.get_barrier_semaphore()
    for peer in peers:
        pl.semaphore_signal(barrier, inc=1, device_id=(row, peer), device_id_type=MESH)
    for peer in row_peers:
        pl.semaphore_signal(barrier, inc=1, device_id=(peer, col), device_id_type=MESH)

    loads = [
        pltpu.make_async_copy(modes_hbm, modes, load_sem.at[0]),
        pltpu.make_async_copy(one_hbm, one, load_sem.at[1]),
        pltpu.make_async_copy(two_hbm, two.at[:, pl.ds(0, N)], load_sem.at[2]),
        pltpu.make_async_copy(three_hbm, three, load_sem.at[3]),
        pltpu.make_async_copy(waves_hbm, waves_ref, load_sem.at[4]),
        pltpu.make_async_copy(polar_hbm, polar_ref, load_sem.at[5]),
        pltpu.make_async_copy(azimuth_hbm, azimuth_ref, load_sem.at[6]),
    ]
    for load in loads:
        load.start()

    padded[...] = jnp.zeros_like(padded)
    i, j = iota((384, 488), 0), iota((384, 488), 1)
    pick = chosen((j // 4 == lax.rem(i, 128)) & (lax.rem(j, 4) == i // 128) & (j < 4 * KL * KL)).astype(BF)
    loads[0].wait()
    for a in range(KL):
        for b in range(KL):
            k = (a * KL + b) * 4
            padded[k : k + 3, 0 : 2 * M] = modes[a, b].astype(F32)
    rows = jnp.dot(pick, padded[...].astype(BF), preferred_element_type=F32)
    picked_re[...] = rows[:, :384].astype(BF)
    moved = pltpu.roll(rows, 768 - M, 1)
    picked_im[...] = moved[:, :384].astype(BF)

    loads[1].wait()
    nt = functools.partial(lax.dot_general, dimension_numbers=NT, preferred_element_type=F32)

    def quarter_turn(x):
        moved = pltpu.roll(x, 4, 1)
        return jnp.where(iota(x.shape, 1) < 4, -moved, moved)

    def along_z(q, carry):
        part = one[pl.ds(pl.multiple_of(q * 256, 256), 256), :]
        x = nt(part, picked_re[...]).reshape(COLS, 8, 384)
        x = (x + quarter_turn(nt(part, picked_im[...]).reshape(COLS, 8, 384))).astype(BF)
        for c in range(3):
            sent[q, :, c] = x[:, :, c * 128 : (c + 1) * 128]

        @pl.when(q == 0)
        def _():
            pl.semaphore_wait(barrier, COLS + ROWS - 2)

        @pl.when(q < 3)
        def _():
            for peer in peers:
                pltpu.make_async_remote_copy(
                    src_ref=sent.at[q, peer], dst_ref=got.at[q, col],
                    send_sem=csend.at[q], recv_sem=crecv.at[q],
                    device_id=(row, peer), device_id_type=MESH,
                ).start()

        @pl.when(q == 3)
        def _():
            def send_col(c, carry):
                for peer in peers:
                    pltpu.make_async_remote_copy(
                        src_ref=sent.at[3, peer, c], dst_ref=got.at[3, col, c],
                        send_sem=csend.at[3 + c], recv_sem=crecv.at[3 + c],
                        device_id=(row, peer), device_id_type=MESH,
                    ).start()
                return carry

            lax.fori_loop(0, 3, send_col, 0)

        got[q, pl.ds(col, 1)] = sent[q, pl.ds(col, 1)]
        return carry

    lax.fori_loop(0, 4, along_z, 0)

    loads[2].wait()

    def fill_two(b, carry):
        base = pl.multiple_of(b * 64, 64)
        half = two[pl.ds(base, 64), 0:N].astype(F32).reshape(8, 8, N)
        two[pl.ds(base, 64), N : 2 * N] = quarter_turn(half).reshape(64, N).astype(BF)
        return carry

    lax.fori_loop(0, 12, fill_two, 0)
    for load in loads[4:]:
        load.wait()

    lane = iota((8, 256), 1)
    wave = jnp.zeros((8, 256), F32)
    polar = jnp.zeros((8, 256), F32)
    azimuth = jnp.zeros((8, 256), F32)
    for m in range(FREQS):
        wave = jnp.where(lane // DIRS == m, waves_ref[m], wave)
    for d in range(DIRS):
        polar = jnp.where(lax.rem(lane, DIRS) == d, polar_ref[d], polar)
        azimuth = jnp.where(lax.rem(lane, DIRS) == d, azimuth_ref[d], azimuth)
    sin_polar = jnp.sin(polar)
    n1 = sin_polar * jnp.cos(azimuth)
    n2 = sin_polar * jnp.sin(azimuth)
    n3 = jnp.cos(polar)
    axes = (n1, n2, n3)
    third = (n1 * n1 + n2 * n2 + n3 * n3) / 3.0
    for c in range(3):
        for e in range(c + 1):
            w = axes[c] * axes[c] - third if e == c else 2.0 * axes[e] * axes[c]
            weights[c, e, :, 0:256] = w
            weights[c, e, :, 256:512] = w
    unit = 2.0 * math.pi / N
    wave_1, one_1, two_1, three_1 = wave[0:1], n1[0:1], n2[0:1], n3[0:1]

    def phases(b, carry):
        base = pl.multiple_of(b * 32, 32)
        index = iota((32, 256), 0) + base
        angle = wave_1 * (one_1 * (index.astype(F32) * unit))
        phase[pl.ds(base, 32), 0:256] = jnp.cos(angle).astype(BF)
        phase[pl.ds(base, 32), 256:512] = (-jnp.sin(angle)).astype(BF)
        part = lax.rem(index, 128)
        y_pos = (row * 32 + part // 4).astype(F32) * unit
        z_pos = (col * 16 + (index // 128) * 4 + lax.rem(part, 4)).astype(F32) * unit
        angle = wave_1 * (two_1 * y_pos) + wave_1 * (three_1 * z_pos)
        cos_yz[pl.ds(base, 32), :] = jnp.cos(angle)
        sin_yz[pl.ds(base, 32), :] = jnp.sin(angle)
        return carry

    lax.fori_loop(0, 16, phases, 0)
    mixed[...] = jnp.zeros_like(mixed)
    spectrum[...] = jnp.zeros_like(spectrum)

    i, j = iota((176, 128), 0), iota((176, 128), 1)
    spread = chosen((j == lax.rem(i, 16) * KL + i // 16) & (lax.rem(i, 16) < KL)).astype(BF)
    turn = chosen(iota((128, 128), 0) == iota((128, 128), 1)).astype(BF)
    loads[3].wait()

    def step(n, carry):
        @pl.when(n < 12)
        def _():
            q = lax.div(n, 3)
            c = n - 3 * q

            @pl.when((q < 3) & (c == 0))
            def _():
                pltpu.make_async_copy(
                    got.at[q, pl.ds(0, COLS - 1)], got.at[q, pl.ds(0, COLS - 1)], crecv.at[q]
                ).wait()

            @pl.when(q == 3)
            def _():
                pltpu.make_async_copy(
                    got.at[3, pl.ds(0, COLS - 1), c], got.at[3, pl.ds(0, COLS - 1), c], crecv.at[3 + c]
                ).wait()

            for t in range(2):
                lines = got[q, t * 16 : t * 16 + 16, c].astype(F32).reshape(128, 128).astype(BF)
                turned = nt(spread, lines).astype(BF)
                tiles = [turned[m * 16 : m * 16 + 16] for m in range(KL)] + [jnp.zeros((16, 128), BF)]
                for k in range(3):
                    for m, tile in enumerate(swapped(tiles[4 * k : 4 * k + 4])):
                        lhs[2 * k + t, m * 16 : m * 16 + 16, :] = tile
            wide = jnp.concatenate([lhs[t] for t in range(6)], 1)
            out = jnp.dot(wide, two[...], preferred_element_type=F32)
            for t in range(8):
                mid[t] = out[:, t * 128 : (t + 1) * 128].astype(BF)

            def regroup_row(p, carry):
                for upper in range(4):
                    tiles = [mid[p * 4 + upper, k * 16 : k * 16 + 16, :] for k in range(4)]
                    for k, tile in enumerate(swapped(tiles)):
                        rsent[n, upper * 4 + k, p] = tile
                return carry

            lax.fori_loop(0, 2, regroup_row, 0)
            for peer in row_peers:
                pltpu.make_async_remote_copy(
                    src_ref=rsent.at[n, peer], dst_ref=rgot.at[n, row],
                    send_sem=rsend.at[n], recv_sem=rrecv.at[n],
                    device_id=(peer, col), device_id_type=MESH,
                ).start()
            rgot[n, pl.ds(row, 1)] = rsent[n, pl.ds(row, 1)]

        @pl.when(n > 2)
        def _():
            e = n - 3
            q = lax.div(e, 3)
            c = e - 3 * q
            odd = lax.rem(q, 2)
            pltpu.make_async_copy(
                rgot.at[e, pl.ds(0, ROWS - 1)], rgot.at[e, pl.ds(0, ROWS - 1)], rrecv.at[e]
            ).wait()
            for p in range(2):
                block = rgot[e, :, p].reshape(256, 128)
                lhs_x[:, p * 256 : (p + 1) * 256] = nt(turn, block).astype(BF)
            field[odd, c] = jnp.dot(lhs_x[...], three[...], preferred_element_type=F32)
            for k in range(2):

                @pl.when(q == 2 * k + 1)
                def _():
                    a = field[0, c].reshape(16, 8, N)
                    b = field[1, c].reshape(16, 8, N)
                    low = iota((16, 8, N), 1) < 4
                    even_y = jnp.where(low, a, pltpu.roll(b, 4, 1))
                    odd_y = jnp.where(low, pltpu.roll(a, 4, 1), b)
                    both = jnp.concatenate([even_y.reshape(16, 1, 8, N), odd_y.reshape(16, 1, 8, N)], 1)
                    vel_ref[c, :, k * 8 : k * 8 + 8, :] = both.reshape(32, 8, N).astype(BF)

            def component(g, carry):
                stress = (field[odd, c] * field[odd, g]).astype(BF)
                lines = jnp.dot(stress, phase[...], preferred_element_type=F32)
                mixed[...] += weights[c, g, 0:1, :] * lines
                return carry

            lax.fori_loop(0, c + 1, component, 0)

            @pl.when(c == 2)
            def _():
                re, im = mixed[:, 0:256], mixed[:, 256:512]
                base = pl.multiple_of(q * 128, 128)
                cosine, sine = cos_yz[pl.ds(base, 128), :], sin_yz[pl.ds(base, 128), :]
                spectrum[0:1, :] += jnp.sum(re * cosine + im * sine, axis=0, keepdims=True)
                spectrum[1:2, :] += jnp.sum(im * cosine - re * sine, axis=0, keepdims=True)
                mixed[...] = jnp.zeros_like(mixed)

        return carry

    lax.fori_loop(0, 15, step, 0)

    sum_re, sum_im = spectrum[0:1, :], spectrum[1:2, :]
    mine = lax.rem(iota((DIRS, 256), 1), DIRS) == iota((DIRS, 256), 0)
    i, j = iota((256, 128), 0) // DIRS, iota((256, 128), 1)
    dot = functools.partial(jnp.dot, preferred_element_type=F32, precision=lax.Precision.HIGHEST)
    per_dir = dot(jnp.where(mine, sum_re, 0.0), chosen(i == j))
    per_dir = per_dir + dot(jnp.where(mine, sum_im, 0.0), chosen(i + FREQS == j))
    for d in range(DIRS):
        fsent[d] = per_dir[d : d + 1]

    for peer in peers:
        pltpu.make_async_remote_copy(
            src_ref=fsent.at[peer], dst_ref=fgot.at[col], send_sem=fsend_sem, recv_sem=frecv_sem,
            device_id=(row, peer), device_id_type=MESH,
        ).start()
    fgot[pl.ds(col, 1)] = fsent[pl.ds(col, 1)]
    pltpu.make_async_copy(
        fgot.at[pl.ds(0, COLS - 1)], fgot.at[pl.ds(0, COLS - 1)], frecv_sem
    ).wait()
    gsent[...] = jnp.sum(fgot[...], axis=0)

    for peer in row_peers:
        pltpu.make_async_remote_copy(
            src_ref=gsent, dst_ref=ggot.at[row], send_sem=gsend_sem, recv_sem=grecv_sem,
            device_id=(peer, col), device_id_type=MESH,
        ).start()
    ggot[pl.ds(row, 1)] = gsent[...][None]
    pltpu.make_async_copy(
        ggot.at[pl.ds(0, ROWS - 1)], ggot.at[pl.ds(0, ROWS - 1)], grecv_sem
    ).wait()
    total = jnp.sum(ggot[...], axis=0)
    lane = iota((1, 128), 1)
    wave = jnp.zeros((1, 128), F32)
    for m in range(FREQS):
        wave = jnp.where(lax.rem(lane, FREQS) == m, waves_ref[m], wave)
    total = total * (wave * wave) / N**1.5
    far_ref[0, 0:1, :] = total[:, 0:FREQS]
    far_ref[0, 1:2, :] = total[:, FREQS : 2 * FREQS]

    for q in range(3):
        pltpu.make_async_copy(
            sent.at[q, pl.ds(0, COLS - 1)], sent.at[q, pl.ds(0, COLS - 1)], csend.at[q]
        ).wait()
    for c in range(3):
        pltpu.make_async_copy(
            sent.at[3, pl.ds(0, COLS - 1), c], sent.at[3, pl.ds(0, COLS - 1), c], csend.at[3 + c]
        ).wait()
    for n in range(12):
        pltpu.make_async_copy(
            rsent.at[n, pl.ds(0, ROWS - 1)], rsent.at[n, pl.ds(0, ROWS - 1)], rsend.at[n]
        ).wait()
    pltpu.make_async_copy(
        fsent.at[pl.ds(0, COLS - 1)], fsent.at[pl.ds(0, COLS - 1)], fsend_sem
    ).wait()
    pltpu.make_async_copy(
        ggot.at[pl.ds(0, ROWS - 1)], ggot.at[pl.ds(0, ROWS - 1)], gsend_sem
    ).wait()


def body(velocity_modes, wavenumbers, polar, azimuth):
    one, two, three = tables()
    hbm = pl.BlockSpec(memory_space=pltpu.HBM)
    dma = pltpu.SemaphoreType.DMA
    return pl.pallas_call(
        kernel,
        out_shape=(
            pltpu.VMEM((3, N // ROWS, N // COLS, N), BF),
            pltpu.VMEM((1, 2, FREQS), F32),
        ),
        in_specs=[hbm] * 7,
        out_specs=(pl.BlockSpec(memory_space=pltpu.VMEM), pl.BlockSpec(memory_space=pltpu.VMEM)),
        scratch_shapes=[
            pltpu.SMEM((FREQS,), F32),
            pltpu.SMEM((DIRS,), F32),
            pltpu.SMEM((DIRS,), F32),
            pltpu.VMEM((KL, KL, 3, 2 * M), BF),
            pltpu.VMEM((488, 768), F32),
            pltpu.VMEM((2 * N, 384), BF),
            pltpu.VMEM((24 * COLS, 2 * N), BF),
            pltpu.VMEM((N, N), BF),
            pltpu.VMEM((384, 384), BF),
            pltpu.VMEM((384, 384), BF),
            pltpu.VMEM((4, COLS, 3, 8, 128), BF),
            pltpu.VMEM((4, COLS, 3, 8, 128), BF),
            pltpu.VMEM((6, 64, 128), BF),
            pltpu.VMEM((8, 64, 128), BF),
            pltpu.VMEM((12, ROWS, 2, 16, 128), BF),
            pltpu.VMEM((12, ROWS, 2, 16, 128), BF),
            pltpu.VMEM((128, N), BF),
            pltpu.VMEM((2, 3, 128, N), F32),
            pltpu.VMEM((N, N), BF),
            pltpu.VMEM((N, 256), F32),
            pltpu.VMEM((N, 256), F32),
            pltpu.VMEM((3, 3, 8, N), F32),
            pltpu.VMEM((128, N), F32),
            pltpu.VMEM((8, 256), F32),
            pltpu.VMEM((COLS, 1, 128), F32),
            pltpu.VMEM((COLS, 1, 128), F32),
            pltpu.VMEM((1, 128), F32),
            pltpu.VMEM((ROWS, 1, 128), F32),
            dma((7,)),
            dma((6,)),
            dma((6,)),
            dma((12,)),
            dma((12,)),
            dma,
            dma,
            dma,
            dma,
        ],
        compiler_params=pltpu.CompilerParams(
            collective_id=0, has_side_effects=True, vmem_limit_bytes=65000000
        ),
    )(jnp.transpose(velocity_modes, (1, 2, 0, 3)), wavenumbers, polar, azimuth, jnp.asarray(one), jnp.asarray(two), jnp.asarray(three))


def solution(mesh):
    in_specs = (P(None, "row", "col", None), P(), P(), P())
    out_specs = (P(None, "row", "col", None), P("col", None, None))
    return jax.shard_map(body, mesh=mesh, in_specs=in_specs, out_specs=out_specs, check_vma=False)
```

```python
import functools
import math

import jax
import jax.numpy as jnp
import numpy as np
from jax import lax
from jax.experimental import pallas as pl
from jax.experimental.pallas import tpu as pltpu
from jax.sharding import PartitionSpec as P

N = 512
M = 352
KX = 176
FREQS = 8
DIRS = 32
ROWS = 16
COLS = 32
KL = 11
BF = jnp.bfloat16
F32 = jnp.float32
MESH = pl.DeviceIdType.MESH
NT = (((1,), (1,)), ((), ()))


def tables():
    cos = np.cos(2.0 * np.pi / N * np.arange(N))
    sin = np.sin(2.0 * np.pi / N * np.arange(N))
    waves = np.arange(M) - M // 2
    grid = (waves[None, :] * np.arange(N)[:, None]) % N
    base = np.stack([cos[grid], sin[grid]], 0).reshape(2, COLS, 2, 8, M)
    one = np.zeros((2, 2, COLS, 8, 384), np.float32)
    one[..., :M] = base.transpose(0, 2, 1, 3, 4)
    one = one.reshape(2, N, 384)
    grid = (waves[:, None] * np.arange(N)[None, :]) % N
    base = np.zeros((2, COLS, 16, N))
    base[:, :, :KL] = np.stack([cos[grid], -sin[grid]], 0).reshape(2, COLS, KL, N)
    two = base.reshape(2, COLS, 2, 8, 2, 8, 2, 16).transpose(2, 1, 0, 3, 4, 6, 7, 5).reshape(2 * N, N)
    half = np.arange(KX)
    grid = (half[:, None] * np.arange(N)[None, :]) % N
    factor = np.where(half == 0, 1.0, 2.0)[:, None]
    base = np.stack([cos[grid], -sin[grid]], 0).astype(jnp.bfloat16).astype(np.float64) * factor
    three = np.zeros((2, ROWS, 16, N), np.float32)
    three[:, :, :KL] = base.reshape(2, ROWS, KL, N)
    three = three.reshape(2 * ROWS * 16, N)
    return [t.astype(jnp.bfloat16) for t in (one, two, three)]


def iota(shape, dim):
    return lax.broadcasted_iota(jnp.int32, shape, dim)


def chosen(condition):
    return jnp.where(condition, 1.0, 0.0)


def swapped(tiles):
    lane = iota((16, 128), 1)
    tiles = list(tiles)
    for bit in range(3):
        step = 1 << bit
        low = lax.rem(lane // step, 2) == 0
        for i in range(8):
            if (i // step) % 2:
                continue
            a, b = tiles[i], tiles[i + step]
            tiles[i] = jnp.where(low, a, pltpu.roll(b, step, 1))
            tiles[i + step] = jnp.where(low, pltpu.roll(a, 128 - step, 1), b)
    return tiles


SHIFTS = (8, 7, 9, 6, 10, 5, 11, 4, 12, 3, 13, 2, 14, 1, 15, 0)


def col_peers(col):
    base = lax.div(col, 16) * 16
    z = col - base
    peers = []
    for shift in SHIFTS:
        there = lax.rem(z + shift, 16)
        peers.append((16 - base) + there)
        if shift:
            peers.append(base + there)
    return peers


def row_peers_of(row):
    x = lax.div(row, 8)
    y = lax.div(row - 8 * x, 2)
    core = row - 8 * x - 2 * y
    peers = []
    for dx in (1, 0):
        for dy in (2, 1, 3, 0):
            there = (1 - x if dx else x) * 8 + lax.rem(y + dy, 4) * 2
            for dc in (1, 0):
                if dx or dy or dc:
                    peers.append(there + (1 - core if dc else core))
    return peers


def kernel(
    modes_hbm, waves_hbm, polar_hbm, azimuth_hbm, one_hbm, two_hbm, three_hbm,
    vel_ref, far_ref,
    waves_ref, polar_ref, azimuth_ref,
    modes, padded, one, two, three, picked_re, picked_im, sent, got, lhs, mid,
    rsent, rgot, lhs_x, field, phase, cos_yz, sin_yz, weights, mixed, spectrum,
    fsent, fgot, gsent, ggot,
    load_sem, csend, crecv, rsend, rrecv, fsend_sem, frecv_sem, gsend_sem, grecv_sem,
):
    row = lax.axis_index("row")
    col = lax.axis_index("col")
    peers = col_peers(col)
    row_peers = row_peers_of(row)

    barrier = pltpu.get_barrier_semaphore()
    for peer in peers:
        pl.semaphore_signal(barrier, inc=1, device_id=(row, peer), device_id_type=MESH)
    for peer in row_peers:
        pl.semaphore_signal(barrier, inc=1, device_id=(peer, col), device_id_type=MESH)

    loads = [
        pltpu.make_async_copy(modes_hbm, modes, load_sem.at[0]),
        pltpu.make_async_copy(one_hbm, one, load_sem.at[1]),
        pltpu.make_async_copy(two_hbm, two.at[:, pl.ds(0, N)], load_sem.at[2]),
        pltpu.make_async_copy(three_hbm, three, load_sem.at[3]),
        pltpu.make_async_copy(waves_hbm, waves_ref, load_sem.at[4]),
        pltpu.make_async_copy(polar_hbm, polar_ref, load_sem.at[5]),
        pltpu.make_async_copy(azimuth_hbm, azimuth_ref, load_sem.at[6]),
    ]
    for load in loads:
        load.start()

    padded[...] = jnp.zeros_like(padded)
    i, j = iota((384, 488), 0), iota((384, 488), 1)
    pick = chosen((j // 4 == lax.rem(i, 128)) & (lax.rem(j, 4) == i // 128) & (j < 4 * KL * KL)).astype(BF)
    loads[0].wait()
    for a in range(KL):
        for b in range(KL):
            k = (a * KL + b) * 4
            padded[k : k + 3, 0 : 2 * M] = modes[a, b].astype(F32)
    rows = jnp.dot(pick, padded[...].astype(BF), preferred_element_type=F32)
    picked_re[...] = rows[:, :384].astype(BF)
    moved = pltpu.roll(rows, 768 - M, 1)
    picked_im[...] = moved[:, :384].astype(BF)

    loads[1].wait()
    nt = functools.partial(lax.dot_general, dimension_numbers=NT, preferred_element_type=F32)

    def along_z(h, carry):
        cosine = one[0, pl.ds(h * 256, 256), :]
        sine = one[1, pl.ds(h * 256, 256), :]
        x_re = nt(cosine, picked_re[...]) - nt(sine, picked_im[...])
        x_im = nt(sine, picked_re[...]) + nt(cosine, picked_im[...])
        x = jnp.concatenate([x_re.reshape(COLS, 8, 384), x_im.reshape(COLS, 8, 384)], 1).astype(BF)
        for c in range(3):
            sent[h * 3 + c] = x[:, :, c * 128 : (c + 1) * 128]

        @pl.when(h == 0)
        def _():
            pl.semaphore_wait(barrier, COLS + ROWS - 2)

        def send_col(c, carry):
            n = h * 3 + c
            for peer in peers:
                pltpu.make_async_remote_copy(
                    src_ref=sent.at[n, peer], dst_ref=got.at[n, col],
                    send_sem=csend.at[n], recv_sem=crecv.at[n],
                    device_id=(row, peer), device_id_type=MESH,
                ).start()
            got[n, pl.ds(col, 1)] = sent[n, pl.ds(col, 1)]
            return carry

        lax.fori_loop(0, 3, send_col, 0)
        return carry

    lax.fori_loop(0, 2, along_z, 0)

    loads[2].wait()

    def fill_two(b, carry):
        base = pl.multiple_of(b * 64, 64)
        half = two[pl.ds(base, 64), 0:N].astype(F32).reshape(4, 2, 8, N)
        other = jnp.concatenate([-half[:, 1:2], half[:, 0:1]], 1)
        two[pl.ds(base, 64), N : 2 * N] = other.reshape(64, N).astype(BF)
        return carry

    lax.fori_loop(0, 16, fill_two, 0)
    for load in loads[4:]:
        load.wait()

    lane = iota((8, 256), 1)
    wave = jnp.zeros((8, 256), F32)
    polar = jnp.zeros((8, 256), F32)
    azimuth = jnp.zeros((8, 256), F32)
    for m in range(FREQS):
        wave = jnp.where(lane // DIRS == m, waves_ref[m], wave)
    for d in range(DIRS):
        polar = jnp.where(lax.rem(lane, DIRS) == d, polar_ref[d], polar)
        azimuth = jnp.where(lax.rem(lane, DIRS) == d, azimuth_ref[d], azimuth)
    sin_polar = jnp.sin(polar)
    n1 = sin_polar * jnp.cos(azimuth)
    n2 = sin_polar * jnp.sin(azimuth)
    n3 = jnp.cos(polar)
    axes = (n1, n2, n3)
    third = (n1 * n1 + n2 * n2 + n3 * n3) / 3.0
    for c in range(3):
        for e in range(c + 1):
            w = axes[c] * axes[c] - third if e == c else 2.0 * axes[e] * axes[c]
            weights[c, e, :, 0:256] = w
            weights[c, e, :, 256:512] = w
    unit = 2.0 * math.pi / N
    wave_1, one_1, two_1, three_1 = wave[0:1], n1[0:1], n2[0:1], n3[0:1]

    def phases(b, carry):
        base = pl.multiple_of(b * 32, 32)
        index = iota((32, 256), 0) + base
        angle = wave_1 * (one_1 * (index.astype(F32) * unit))
        phase[pl.ds(base, 32), 0:256] = jnp.cos(angle).astype(BF)
        phase[pl.ds(base, 32), 256:512] = (-jnp.sin(angle)).astype(BF)
        part = lax.rem(index, 256)
        y_pos = (row * 32 + part // 8).astype(F32) * unit
        z_pos = (col * 16 + (index // 256) * 8 + lax.rem(part, 8)).astype(F32) * unit
        angle = wave_1 * (two_1 * y_pos) + wave_1 * (three_1 * z_pos)
        cos_yz[pl.ds(base, 32), :] = jnp.cos(angle)
        sin_yz[pl.ds(base, 32), :] = jnp.sin(angle)
        return carry

    lax.fori_loop(0, 16, phases, 0)
    mixed[...] = jnp.zeros_like(mixed)
    spectrum[...] = jnp.zeros_like(spectrum)

    i, j = iota((176, 128), 0), iota((176, 128), 1)
    spread = chosen((j == lax.rem(i, 16) * KL + i // 16) & (lax.rem(i, 16) < KL)).astype(BF)
    turn = chosen(iota((128, 128), 0) == iota((128, 128), 1)).astype(BF)
    loads[3].wait()

    def step(n, carry):
        @pl.when(n < 6)
        def _():
            pltpu.make_async_copy(
                got.at[n, pl.ds(0, COLS - 1)], got.at[n, pl.ds(0, COLS - 1)], crecv.at[n]
            ).wait()

            def regroup(pair, carry):
                for k in range(2):
                    t = pair * 2 + k
                    lines = got[n, pl.ds(t * 8, 8)].reshape(128, 128)
                    turned = nt(spread, lines).astype(BF)
                    zero = jnp.zeros((16, 128), BF)
                    tiles = [turned[m * 16 : m * 16 + 16] for m in range(KL)] + [zero] * (16 - KL)
                    for m, tile in enumerate(swapped(tiles[:8])):
                        lhs[t, m * 16 : m * 16 + 16, :] = tile
                    for m, tile in enumerate(swapped(tiles[8:])):
                        lhs[t + 4, m * 16 : m * 16 + 16, :] = tile
                return carry

            lax.fori_loop(0, 2, regroup, 0)
            wide = jnp.concatenate([lhs[t] for t in range(8)], 1)
            out = jnp.dot(wide, two[...], preferred_element_type=F32)
            for t in range(8):
                mid[t] = out[:, t * 128 : (t + 1) * 128].astype(BF)

            def regroup_row(part, carry):
                for upper in range(2):
                    for y_upper in range(2):
                        t = part * 4 + upper * 2 + y_upper
                        tiles = [mid[t, k * 16 : k * 16 + 16, :] for k in range(8)]
                        for k, tile in enumerate(swapped(tiles)):
                            rsent[n, upper * 8 + k, part * 2 + y_upper] = tile
                return carry

            lax.fori_loop(0, 2, regroup_row, 0)
            for peer in row_peers:
                pltpu.make_async_remote_copy(
                    src_ref=rsent.at[n, peer], dst_ref=rgot.at[n, row],
                    send_sem=rsend.at[n], recv_sem=rrecv.at[n],
                    device_id=(peer, col), device_id_type=MESH,
                ).start()
            rgot[n, pl.ds(row, 1)] = rsent[n, pl.ds(row, 1)]

        @pl.when(n > 0)
        def _():
            e = n - 1
            h = lax.div(e, 3)
            c = e - 3 * h
            pltpu.make_async_copy(
                rgot.at[e, pl.ds(0, ROWS - 1)], rgot.at[e, pl.ds(0, ROWS - 1)], rrecv.at[e]
            ).wait()
            for y_upper in range(2):
                for p in range(2):
                    block = rgot[e, :, p * 2 + y_upper].reshape(256, 128)
                    lhs_x[y_upper * 128 : (y_upper + 1) * 128, p * 256 : (p + 1) * 256] = nt(turn, block).astype(BF)
            field[c] = jnp.dot(lhs_x[...], three[...], preferred_element_type=F32)
            for k in range(2):

                @pl.when(h == k)
                def _():
                    vel_ref[c, :, k * 8 : k * 8 + 8, :] = field[c].reshape(32, 8, N).astype(BF)

            def component(g, carry):
                stress = (field[c] * field[g]).astype(BF)
                lines = jnp.dot(stress, phase[...], preferred_element_type=F32)
                mixed[...] += weights[c, g, 0:1, :] * lines
                return carry

            lax.fori_loop(0, c + 1, component, 0)

            @pl.when(c == 2)
            def _():
                re, im = mixed[:, 0:256], mixed[:, 256:512]
                cosine, sine = cos_yz[pl.ds(h * 256, 256), :], sin_yz[pl.ds(h * 256, 256), :]
                spectrum[0:1, :] += jnp.sum(re * cosine + im * sine, axis=0, keepdims=True)
                spectrum[1:2, :] += jnp.sum(im * cosine - re * sine, axis=0, keepdims=True)
                mixed[...] = jnp.zeros_like(mixed)

        return carry

    lax.fori_loop(0, 7, step, 0)

    sum_re, sum_im = spectrum[0:1, :], spectrum[1:2, :]
    mine = lax.rem(iota((DIRS, 256), 1), DIRS) == iota((DIRS, 256), 0)
    i, j = iota((256, 128), 0) // DIRS, iota((256, 128), 1)
    dot = functools.partial(jnp.dot, preferred_element_type=F32, precision=lax.Precision.HIGHEST)
    per_dir = dot(jnp.where(mine, sum_re, 0.0), chosen(i == j))
    per_dir = per_dir + dot(jnp.where(mine, sum_im, 0.0), chosen(i + FREQS == j))
    for d in range(DIRS):
        fsent[d] = per_dir[d : d + 1]

    for peer in peers:
        pltpu.make_async_remote_copy(
            src_ref=fsent.at[peer], dst_ref=fgot.at[col], send_sem=fsend_sem, recv_sem=frecv_sem,
            device_id=(row, peer), device_id_type=MESH,
        ).start()
    fgot[pl.ds(col, 1)] = fsent[pl.ds(col, 1)]
    pltpu.make_async_copy(
        fgot.at[pl.ds(0, COLS - 1)], fgot.at[pl.ds(0, COLS - 1)], frecv_sem
    ).wait()
    gsent[...] = jnp.sum(fgot[...], axis=0)

    for peer in row_peers:
        pltpu.make_async_remote_copy(
            src_ref=gsent, dst_ref=ggot.at[row], send_sem=gsend_sem, recv_sem=grecv_sem,
            device_id=(peer, col), device_id_type=MESH,
        ).start()
    ggot[pl.ds(row, 1)] = gsent[...][None]
    pltpu.make_async_copy(
        ggot.at[pl.ds(0, ROWS - 1)], ggot.at[pl.ds(0, ROWS - 1)], grecv_sem
    ).wait()
    total = jnp.sum(ggot[...], axis=0)
    lane = iota((1, 128), 1)
    wave = jnp.zeros((1, 128), F32)
    for m in range(FREQS):
        wave = jnp.where(lax.rem(lane, FREQS) == m, waves_ref[m], wave)
    total = total * (wave * wave) / N**1.5
    far_ref[0, 0:1, :] = total[:, 0:FREQS]
    far_ref[0, 1:2, :] = total[:, FREQS : 2 * FREQS]

    for c in range(6):
        pltpu.make_async_copy(
            sent.at[c, pl.ds(0, COLS - 1)], sent.at[c, pl.ds(0, COLS - 1)], csend.at[c]
        ).wait()
        pltpu.make_async_copy(
            rsent.at[c, pl.ds(0, ROWS - 1)], rsent.at[c, pl.ds(0, ROWS - 1)], rsend.at[c]
        ).wait()
    pltpu.make_async_copy(
        fsent.at[pl.ds(0, COLS - 1)], fsent.at[pl.ds(0, COLS - 1)], fsend_sem
    ).wait()
    pltpu.make_async_copy(
        ggot.at[pl.ds(0, ROWS - 1)], ggot.at[pl.ds(0, ROWS - 1)], gsend_sem
    ).wait()


def body(velocity_modes, wavenumbers, polar, azimuth):
    one, two, three = tables()
    hbm = pl.BlockSpec(memory_space=pltpu.HBM)
    dma = pltpu.SemaphoreType.DMA
    return pl.pallas_call(
        kernel,
        out_shape=(
            pltpu.VMEM((3, N // ROWS, N // COLS, N), BF),
            pltpu.VMEM((1, 2, FREQS), F32),
        ),
        in_specs=[hbm] * 7,
        out_specs=(pl.BlockSpec(memory_space=pltpu.VMEM), pl.BlockSpec(memory_space=pltpu.VMEM)),
        scratch_shapes=[
            pltpu.SMEM((FREQS,), F32),
            pltpu.SMEM((DIRS,), F32),
            pltpu.SMEM((DIRS,), F32),
            pltpu.VMEM((KL, KL, 3, 2 * M), BF),
            pltpu.VMEM((488, 768), F32),
            pltpu.VMEM((2, N, 384), BF),
            pltpu.VMEM((2 * N, 2 * N), BF),
            pltpu.VMEM((N, N), BF),
            pltpu.VMEM((384, 384), BF),
            pltpu.VMEM((384, 384), BF),
            pltpu.VMEM((6, COLS, 16, 128), BF),
            pltpu.VMEM((6, COLS, 16, 128), BF),
            pltpu.VMEM((8, 128, 128), BF),
            pltpu.VMEM((8, 128, 128), BF),
            pltpu.VMEM((6, ROWS, 4, 16, 128), BF),
            pltpu.VMEM((6, ROWS, 4, 16, 128), BF),
            pltpu.VMEM((256, N), BF),
            pltpu.VMEM((3, 256, N), F32),
            pltpu.VMEM((N, N), BF),
            pltpu.VMEM((N, 256), F32),
            pltpu.VMEM((N, 256), F32),
            pltpu.VMEM((3, 3, 8, N), F32),
            pltpu.VMEM((256, N), F32),
            pltpu.VMEM((8, 256), F32),
            pltpu.VMEM((COLS, 1, 128), F32),
            pltpu.VMEM((COLS, 1, 128), F32),
            pltpu.VMEM((1, 128), F32),
            pltpu.VMEM((ROWS, 1, 128), F32),
            dma((7,)),
            dma((6,)),
            dma((6,)),
            dma((6,)),
            dma((6,)),
            dma,
            dma,
            dma,
            dma,
        ],
        compiler_params=pltpu.CompilerParams(
            collective_id=0, has_side_effects=True, vmem_limit_bytes=65000000
        ),
    )(jnp.transpose(velocity_modes, (1, 2, 0, 3)), wavenumbers, polar, azimuth, jnp.asarray(one), jnp.asarray(two), jnp.asarray(three))


def solution(mesh):
    in_specs = (P(None, "row", "col", None), P(), P(), P())
    out_specs = (P(None, "row", "col", None), P("col", None, None))
    return jax.shard_map(body, mesh=mesh, in_specs=in_specs, out_specs=out_specs, check_vma=False)
```

```python
import functools
import math

import jax
import jax.numpy as jnp
import numpy as np
from jax import lax
from jax.experimental import pallas as pl
from jax.experimental.pallas import tpu as pltpu
from jax.sharding import PartitionSpec as P

N = 512
M = 352
KX = 176
FREQS = 8
DIRS = 32
ROWS = 16
COLS = 32
KL = 11
BF = jnp.bfloat16
F32 = jnp.float32
MESH = pl.DeviceIdType.MESH
NT = (((1,), (1,)), ((), ()))


def tables():
    cos = np.cos(2.0 * np.pi / N * np.arange(N))
    sin = np.sin(2.0 * np.pi / N * np.arange(N))
    waves = np.arange(M) - M // 2
    grid = (waves[None, :] * np.arange(N)[:, None]) % N
    base = np.stack([cos[grid], sin[grid]], 0).reshape(2, COLS, 2, 8, M)
    one = np.zeros((2, 2, COLS, 8, 384), np.float32)
    one[..., :M] = base.transpose(0, 2, 1, 3, 4)
    one = one.reshape(2, N, 384)
    grid = (waves[:, None] * np.arange(N)[None, :]) % N
    base = np.zeros((2, COLS, 16, N))
    base[:, :, :KL] = np.stack([cos[grid], -sin[grid]], 0).reshape(2, COLS, KL, N)
    two = base.reshape(2, COLS, 2, 8, 2, 8, 2, 16).transpose(2, 1, 0, 3, 4, 6, 7, 5).reshape(2 * N, N)
    half = np.arange(KX)
    grid = (half[:, None] * np.arange(N)[None, :]) % N
    factor = np.where(half == 0, 1.0, 2.0)[:, None]
    base = np.stack([cos[grid], -sin[grid]], 0).astype(jnp.bfloat16).astype(np.float64) * factor
    three = np.zeros((2, ROWS, 16, N), np.float32)
    three[:, :, :KL] = base.reshape(2, ROWS, KL, N)
    three = three.reshape(2 * ROWS * 16, N)
    return [t.astype(jnp.bfloat16) for t in (one, two, three)]


def iota(shape, dim):
    return lax.broadcasted_iota(jnp.int32, shape, dim)


def chosen(condition):
    return jnp.where(condition, 1.0, 0.0)


def swapped(tiles):
    lane = iota((16, 128), 1)
    tiles = list(tiles)
    for bit in range(3):
        step = 1 << bit
        low = lax.rem(lane // step, 2) == 0
        for i in range(8):
            if (i // step) % 2:
                continue
            a, b = tiles[i], tiles[i + step]
            tiles[i] = jnp.where(low, a, pltpu.roll(b, step, 1))
            tiles[i + step] = jnp.where(low, pltpu.roll(a, 128 - step, 1), b)
    return tiles


SHIFTS = (8, 7, 9, 6, 10, 5, 11, 4, 12, 3, 13, 2, 14, 1, 15, 0)


def col_peers(col):
    base = lax.div(col, 16) * 16
    z = col - base
    peers = []
    for shift in SHIFTS:
        there = lax.rem(z + shift, 16)
        peers.append((16 - base) + there)
        if shift:
            peers.append(base + there)
    return peers


def kernel(
    modes_hbm, waves_hbm, polar_hbm, azimuth_hbm, one_hbm, two_hbm, three_hbm,
    vel_ref, far_ref,
    waves_ref, polar_ref, azimuth_ref,
    modes, padded, one, two, three, picked_re, picked_im, sent, got, lhs, mid,
    rsent, rgot, lhs_x, field, phase, cos_yz, sin_yz, weights, mixed, spectrum,
    fsent, fgot, gsent, ggot,
    load_sem, csend, crecv, rsend, rrecv, fsend_sem, frecv_sem, gsend_sem, grecv_sem,
):
    row = lax.axis_index("row")
    col = lax.axis_index("col")
    peers = col_peers(col)
    row_peers = [lax.rem(row + k, ROWS) for k in range(1, ROWS)]

    barrier = pltpu.get_barrier_semaphore()
    for peer in peers:
        pl.semaphore_signal(barrier, inc=1, device_id=(row, peer), device_id_type=MESH)
    for peer in row_peers:
        pl.semaphore_signal(barrier, inc=1, device_id=(peer, col), device_id_type=MESH)

    loads = [
        pltpu.make_async_copy(modes_hbm, modes, load_sem.at[0]),
        pltpu.make_async_copy(one_hbm, one, load_sem.at[1]),
        pltpu.make_async_copy(two_hbm, two.at[:, pl.ds(0, N)], load_sem.at[2]),
        pltpu.make_async_copy(three_hbm, three, load_sem.at[3]),
        pltpu.make_async_copy(waves_hbm, waves_ref, load_sem.at[4]),
        pltpu.make_async_copy(polar_hbm, polar_ref, load_sem.at[5]),
        pltpu.make_async_copy(azimuth_hbm, azimuth_ref, load_sem.at[6]),
    ]
    for load in loads:
        load.start()

    padded[...] = jnp.zeros_like(padded)
    i, j = iota((384, 488), 0), iota((384, 488), 1)
    pick = chosen((j // 4 == lax.rem(i, 128)) & (lax.rem(j, 4) == i // 128) & (j < 4 * KL * KL)).astype(BF)
    loads[0].wait()
    for a in range(KL):
        for b in range(KL):
            k = (a * KL + b) * 4
            padded[k : k + 3, 0 : 2 * M] = modes[a, b].astype(F32)
    rows = jnp.dot(pick, padded[...].astype(BF), preferred_element_type=F32)
    picked_re[...] = rows[:, :384].astype(BF)
    moved = pltpu.roll(rows, 768 - M, 1)
    picked_im[...] = moved[:, :384].astype(BF)

    loads[1].wait()
    nt = functools.partial(lax.dot_general, dimension_numbers=NT, preferred_element_type=F32)

    def along_z(h, carry):
        cosine = one[0, pl.ds(h * 256, 256), :]
        sine = one[1, pl.ds(h * 256, 256), :]
        x_re = nt(cosine, picked_re[...]) - nt(sine, picked_im[...])
        x_im = nt(sine, picked_re[...]) + nt(cosine, picked_im[...])
        x = jnp.concatenate([x_re.reshape(COLS, 8, 384), x_im.reshape(COLS, 8, 384)], 1).astype(BF)
        for c in range(3):
            sent[h * 3 + c] = x[:, :, c * 128 : (c + 1) * 128]

        @pl.when(h == 0)
        def _():
            pl.semaphore_wait(barrier, COLS + ROWS - 2)

        def send_col(c, carry):
            n = h * 3 + c
            for peer in peers:
                pltpu.make_async_remote_copy(
                    src_ref=sent.at[n, peer], dst_ref=got.at[n, col],
                    send_sem=csend.at[n], recv_sem=crecv.at[n],
                    device_id=(row, peer), device_id_type=MESH,
                ).start()
            got[n, pl.ds(col, 1)] = sent[n, pl.ds(col, 1)]
            return carry

        lax.fori_loop(0, 3, send_col, 0)
        return carry

    lax.fori_loop(0, 2, along_z, 0)

    loads[2].wait()

    def fill_two(b, carry):
        base = pl.multiple_of(b * 64, 64)
        half = two[pl.ds(base, 64), 0:N].astype(F32).reshape(4, 2, 8, N)
        other = jnp.concatenate([-half[:, 1:2], half[:, 0:1]], 1)
        two[pl.ds(base, 64), N : 2 * N] = other.reshape(64, N).astype(BF)
        return carry

    lax.fori_loop(0, 16, fill_two, 0)
    for load in loads[4:]:
        load.wait()

    lane = iota((8, 256), 1)
    wave = jnp.zeros((8, 256), F32)
    polar = jnp.zeros((8, 256), F32)
    azimuth = jnp.zeros((8, 256), F32)
    for m in range(FREQS):
        wave = jnp.where(lane // DIRS == m, waves_ref[m], wave)
    for d in range(DIRS):
        polar = jnp.where(lax.rem(lane, DIRS) == d, polar_ref[d], polar)
        azimuth = jnp.where(lax.rem(lane, DIRS) == d, azimuth_ref[d], azimuth)
    sin_polar = jnp.sin(polar)
    n1 = sin_polar * jnp.cos(azimuth)
    n2 = sin_polar * jnp.sin(azimuth)
    n3 = jnp.cos(polar)
    axes = (n1, n2, n3)
    third = (n1 * n1 + n2 * n2 + n3 * n3) / 3.0
    for c in range(3):
        for e in range(c + 1):
            w = axes[c] * axes[c] - third if e == c else 2.0 * axes[e] * axes[c]
            weights[c, e, :, 0:256] = w
            weights[c, e, :, 256:512] = w
    unit = 2.0 * math.pi / N
    wave_1, one_1, two_1, three_1 = wave[0:1], n1[0:1], n2[0:1], n3[0:1]

    def phases(b, carry):
        base = pl.multiple_of(b * 32, 32)
        index = iota((32, 256), 0) + base
        angle = wave_1 * (one_1 * (index.astype(F32) * unit))
        phase[pl.ds(base, 32), 0:256] = jnp.cos(angle).astype(BF)
        phase[pl.ds(base, 32), 256:512] = (-jnp.sin(angle)).astype(BF)
        part = lax.rem(index, 256)
        y_pos = (row * 32 + part // 8).astype(F32) * unit
        z_pos = (col * 16 + (index // 256) * 8 + lax.rem(part, 8)).astype(F32) * unit
        angle = wave_1 * (two_1 * y_pos) + wave_1 * (three_1 * z_pos)
        cos_yz[pl.ds(base, 32), :] = jnp.cos(angle)
        sin_yz[pl.ds(base, 32), :] = jnp.sin(angle)
        return carry

    lax.fori_loop(0, 16, phases, 0)
    mixed[...] = jnp.zeros_like(mixed)
    spectrum[...] = jnp.zeros_like(spectrum)

    i, j = iota((176, 128), 0), iota((176, 128), 1)
    spread = chosen((j == lax.rem(i, 16) * KL + i // 16) & (lax.rem(i, 16) < KL)).astype(BF)
    turn = chosen(iota((128, 128), 0) == iota((128, 128), 1)).astype(BF)
    loads[3].wait()

    def step(n, carry):
        @pl.when(n < 6)
        def _():
            pltpu.make_async_copy(
                got.at[n, pl.ds(0, COLS - 1)], got.at[n, pl.ds(0, COLS - 1)], crecv.at[n]
            ).wait()

            def regroup(pair, carry):
                for k in range(2):
                    t = pair * 2 + k
                    lines = got[n, pl.ds(t * 8, 8)].reshape(128, 128)
                    turned = nt(spread, lines).astype(BF)
                    zero = jnp.zeros((16, 128), BF)
                    tiles = [turned[m * 16 : m * 16 + 16] for m in range(KL)] + [zero] * (16 - KL)
                    for m, tile in enumerate(swapped(tiles[:8])):
                        lhs[t, m * 16 : m * 16 + 16, :] = tile
                    for m, tile in enumerate(swapped(tiles[8:])):
                        lhs[t + 4, m * 16 : m * 16 + 16, :] = tile
                return carry

            lax.fori_loop(0, 2, regroup, 0)
            wide = jnp.concatenate([lhs[t] for t in range(8)], 1)
            out = jnp.dot(wide, two[...], preferred_element_type=F32)
            for t in range(8):
                mid[t] = out[:, t * 128 : (t + 1) * 128].astype(BF)

            def regroup_row(part, carry):
                for upper in range(2):
                    for y_upper in range(2):
                        t = part * 4 + upper * 2 + y_upper
                        tiles = [mid[t, k * 16 : k * 16 + 16, :] for k in range(8)]
                        for k, tile in enumerate(swapped(tiles)):
                            rsent[n, upper * 8 + k, part * 2 + y_upper] = tile
                return carry

            lax.fori_loop(0, 2, regroup_row, 0)
            for peer in row_peers:
                pltpu.make_async_remote_copy(
                    src_ref=rsent.at[n, peer], dst_ref=rgot.at[n, row],
                    send_sem=rsend.at[n], recv_sem=rrecv.at[n],
                    device_id=(peer, col), device_id_type=MESH,
                ).start()
            rgot[n, pl.ds(row, 1)] = rsent[n, pl.ds(row, 1)]

        @pl.when(n > 1)
        def _():
            e = n - 2
            h = lax.div(e, 3)
            c = e - 3 * h
            pltpu.make_async_copy(
                rgot.at[e, pl.ds(0, ROWS - 1)], rgot.at[e, pl.ds(0, ROWS - 1)], rrecv.at[e]
            ).wait()
            for y_upper in range(2):
                for p in range(2):
                    block = rgot[e, :, p * 2 + y_upper].reshape(256, 128)
                    lhs_x[y_upper * 128 : (y_upper + 1) * 128, p * 256 : (p + 1) * 256] = nt(turn, block).astype(BF)
            field[c] = jnp.dot(lhs_x[...], three[...], preferred_element_type=F32)
            for k in range(2):

                @pl.when(h == k)
                def _():
                    vel_ref[c, :, k * 8 : k * 8 + 8, :] = field[c].reshape(32, 8, N).astype(BF)

            def component(g, carry):
                stress = (field[c] * field[g]).astype(BF)
                lines = jnp.dot(stress, phase[...], preferred_element_type=F32)
                mixed[...] += weights[c, g, 0:1, :] * lines
                return carry

            lax.fori_loop(0, c + 1, component, 0)

            @pl.when(c == 2)
            def _():
                re, im = mixed[:, 0:256], mixed[:, 256:512]
                cosine, sine = cos_yz[pl.ds(h * 256, 256), :], sin_yz[pl.ds(h * 256, 256), :]
                spectrum[0:1, :] += jnp.sum(re * cosine + im * sine, axis=0, keepdims=True)
                spectrum[1:2, :] += jnp.sum(im * cosine - re * sine, axis=0, keepdims=True)
                mixed[...] = jnp.zeros_like(mixed)

        return carry

    lax.fori_loop(0, 8, step, 0)

    sum_re, sum_im = spectrum[0:1, :], spectrum[1:2, :]
    mine = lax.rem(iota((DIRS, 256), 1), DIRS) == iota((DIRS, 256), 0)
    i, j = iota((256, 128), 0) // DIRS, iota((256, 128), 1)
    dot = functools.partial(jnp.dot, preferred_element_type=F32, precision=lax.Precision.HIGHEST)
    per_dir = dot(jnp.where(mine, sum_re, 0.0), chosen(i == j))
    per_dir = per_dir + dot(jnp.where(mine, sum_im, 0.0), chosen(i + FREQS == j))
    for d in range(DIRS):
        fsent[d] = per_dir[d : d + 1]

    for peer in peers:
        pltpu.make_async_remote_copy(
            src_ref=fsent.at[peer], dst_ref=fgot.at[col], send_sem=fsend_sem, recv_sem=frecv_sem,
            device_id=(row, peer), device_id_type=MESH,
        ).start()
    fgot[pl.ds(col, 1)] = fsent[pl.ds(col, 1)]
    pltpu.make_async_copy(
        fgot.at[pl.ds(0, COLS - 1)], fgot.at[pl.ds(0, COLS - 1)], frecv_sem
    ).wait()
    gsent[...] = jnp.sum(fgot[...], axis=0)

    for peer in row_peers:
        pltpu.make_async_remote_copy(
            src_ref=gsent, dst_ref=ggot.at[row], send_sem=gsend_sem, recv_sem=grecv_sem,
            device_id=(peer, col), device_id_type=MESH,
        ).start()
    ggot[pl.ds(row, 1)] = gsent[...][None]
    pltpu.make_async_copy(
        ggot.at[pl.ds(0, ROWS - 1)], ggot.at[pl.ds(0, ROWS - 1)], grecv_sem
    ).wait()
    total = jnp.sum(ggot[...], axis=0)
    lane = iota((1, 128), 1)
    wave = jnp.zeros((1, 128), F32)
    for m in range(FREQS):
        wave = jnp.where(lax.rem(lane, FREQS) == m, waves_ref[m], wave)
    total = total * (wave * wave) / N**1.5
    far_ref[0, 0:1, :] = total[:, 0:FREQS]
    far_ref[0, 1:2, :] = total[:, FREQS : 2 * FREQS]

    for c in range(6):
        pltpu.make_async_copy(
            sent.at[c, pl.ds(0, COLS - 1)], sent.at[c, pl.ds(0, COLS - 1)], csend.at[c]
        ).wait()
        pltpu.make_async_copy(
            rsent.at[c, pl.ds(0, ROWS - 1)], rsent.at[c, pl.ds(0, ROWS - 1)], rsend.at[c]
        ).wait()
    pltpu.make_async_copy(
        fsent.at[pl.ds(0, COLS - 1)], fsent.at[pl.ds(0, COLS - 1)], fsend_sem
    ).wait()
    pltpu.make_async_copy(
        ggot.at[pl.ds(0, ROWS - 1)], ggot.at[pl.ds(0, ROWS - 1)], gsend_sem
    ).wait()


def body(velocity_modes, wavenumbers, polar, azimuth):
    one, two, three = tables()
    hbm = pl.BlockSpec(memory_space=pltpu.HBM)
    dma = pltpu.SemaphoreType.DMA
    return pl.pallas_call(
        kernel,
        out_shape=(
            pltpu.VMEM((3, N // ROWS, N // COLS, N), BF),
            pltpu.VMEM((1, 2, FREQS), F32),
        ),
        in_specs=[hbm] * 7,
        out_specs=(pl.BlockSpec(memory_space=pltpu.VMEM), pl.BlockSpec(memory_space=pltpu.VMEM)),
        scratch_shapes=[
            pltpu.SMEM((FREQS,), F32),
            pltpu.SMEM((DIRS,), F32),
            pltpu.SMEM((DIRS,), F32),
            pltpu.VMEM((KL, KL, 3, 2 * M), BF),
            pltpu.VMEM((488, 768), F32),
            pltpu.VMEM((2, N, 384), BF),
            pltpu.VMEM((2 * N, 2 * N), BF),
            pltpu.VMEM((N, N), BF),
            pltpu.VMEM((384, 384), BF),
            pltpu.VMEM((384, 384), BF),
            pltpu.VMEM((6, COLS, 16, 128), BF),
            pltpu.VMEM((6, COLS, 16, 128), BF),
            pltpu.VMEM((8, 128, 128), BF),
            pltpu.VMEM((8, 128, 128), BF),
            pltpu.VMEM((6, ROWS, 4, 16, 128), BF),
            pltpu.VMEM((6, ROWS, 4, 16, 128), BF),
            pltpu.VMEM((256, N), BF),
            pltpu.VMEM((3, 256, N), F32),
            pltpu.VMEM((N, N), BF),
            pltpu.VMEM((N, 256), F32),
            pltpu.VMEM((N, 256), F32),
            pltpu.VMEM((3, 3, 8, N), F32),
            pltpu.VMEM((256, N), F32),
            pltpu.VMEM((8, 256), F32),
            pltpu.VMEM((COLS, 1, 128), F32),
            pltpu.VMEM((COLS, 1, 128), F32),
            pltpu.VMEM((1, 128), F32),
            pltpu.VMEM((ROWS, 1, 128), F32),
            dma((7,)),
            dma((6,)),
            dma((6,)),
            dma((6,)),
            dma((6,)),
            dma,
            dma,
            dma,
            dma,
        ],
        compiler_params=pltpu.CompilerParams(
            collective_id=0, has_side_effects=True, vmem_limit_bytes=65000000
        ),
    )(jnp.transpose(velocity_modes, (1, 2, 0, 3)), wavenumbers, polar, azimuth, jnp.asarray(one), jnp.asarray(two), jnp.asarray(three))


def solution(mesh):
    in_specs = (P(None, "row", "col", None), P(), P(), P())
    out_specs = (P(None, "row", "col", None), P("col", None, None))
    return jax.shard_map(body, mesh=mesh, in_specs=in_specs, out_specs=out_specs, check_vma=False)
```
